256 devices in a mesh: mem: 4 (over x), cell: 64 (over y, z, core).
Axes of the slice: x: 4, y: 4, z: 8, core: 2. Of those that a mesh axis runs over, the one named last changes fastest.
Arguments:
- state: bfloat16 [131072, 40, 120], P('cell', 'mem'), may hold values from -6 to 6
- vertical_weight: bfloat16 [65536, 120], P('cell'), may hold values from -0.5 to 0.5
- horizontal_weight: float32 [65536, 4], P('cell'), may hold values from 0.05 to 0.45
- obs_slot: int32 [65536, 4], P('cell'), may hold values from 0 to 4095, as said below
- request_cell: int32 [64, 4096], P('cell'), may hold values from 0 to 2047
- obs_value: float32 [65536], P('cell'), may hold values from -6 to 6
- obs_error: float32 [65536], P('cell'), may hold values from 0.5 to 2
- obs_region: int32 [65536], P('cell'), may hold values from 0 to 511, as said below
Outputs:
- cov_matrix: float32 [512, 40, 40], P('cell', 'mem')
- innovation_proj: float32 [512, 40], P('cell', 'mem')
The draws below stay inside these ranges and needn't reach their ends.
Inputs may be any that keep to these rules, and one draw needn't show every extreme that they name: `obs_slot`: within one owner's 1024 observations all 4096 slots differ, so every slot is used: 1024 ask the owner's own patch and 768 each of the four patches at distance 1 and 2. `obs_region`: an observation's region is one of the 8 regions of its owner's patch or of the patches just before or after it (indices wrap); patch p holds regions p * 8 to p * 8 + 7.
All inputs are finite; a program needn't handle non-finite values.
Results may differ from the reference program's by a relative error of at most 0.0003.
Values may be sent and summed in bfloat16 or wider, within the bound.
No kernel may reach another device: no remote copies, remote signals or barrier semaphores. Data moves between devices by JAX's collectives and lax.ppermute only.
A program may use at most 128 MiB of HBM per device.

```python
import math
import jax
import jax.numpy as jnp
from jax import lax

MEMBERS = 40
LEV = 120
NEIGH = 4
CELL_DEV = 2048
OBS_DEV = 1024
REG_DEV = 8
HALO_CAP = 768
OWN_CAP = 1024
CELLS = 131072
OBS = 65536
REGIONS = 512
N_CELL = 64


def routing(key):
    base = jax.random.fold_in(key, 71)

    def one_owner(owner_key):
        key_perm, key_cell = jax.random.split(owner_key, 2)
        total = 4 * OBS_DEV
        chosen = jax.random.permutation(key_perm, total).astype(jnp.int32).reshape(OBS_DEV, NEIGH)
        cells = jax.random.randint(key_cell, (total,), 0, CELL_DEV).astype(jnp.int32)
        return (chosen, cells)
    keys = jax.random.split(base, N_CELL)
    chosen, cells = jax.vmap(one_owner)(keys)
    return (chosen.reshape(OBS, NEIGH), cells.reshape(N_CELL, 4 * OBS_DEV))


def draw_obs_slot(key, part):
    return routing(key)[0]


def draw_request_cell(key, part):
    return routing(key)[1]


def draw_obs_region(key, part):
    key_side, key_within = jax.random.split(jax.random.fold_in(key, 53), 2)
    code = jax.random.randint(key_side, (N_CELL, OBS_DEV), 0, 4).astype(jnp.int32)
    moves = jnp.array([-1, 0, 0, 1], dtype=jnp.int32)[code]
    owner = jnp.arange(N_CELL, dtype=jnp.int32)[:, None]
    patch = jnp.mod(owner + moves, N_CELL).astype(jnp.int32)
    within = jax.random.randint(key_within, (N_CELL, OBS_DEV), 0, REG_DEV).astype(jnp.int32)
    return (patch * REG_DEV + within).reshape(OBS).astype(jnp.int32)


def block_scale(rng, shape, shards, least, top_value):
    def one(position, parts):
        heights = jax.random.uniform(jax.random.fold_in(jax.random.fold_in(rng, 6), position), (parts,), jnp.float32, least / len(shards), top_value / len(shards))
        return jnp.repeat(jnp.exp(heights), shape[position] // parts).reshape((-1,) + (1,) * (len(shape) - position - 1))

    factor_of = one(*shards[0])
    for cut in shards[1:]:
        factor_of = factor_of * one(*cut)
    return factor_of


def bell_draw(rng, shape, scale, most, shards=(), held_as=jnp.bfloat16):
    loudness = block_scale(rng, shape, shards, -0.22, 0.18) if shards else 1.0
    values = jax.random.normal(rng, shape, jnp.float32) * scale * loudness
    return jnp.minimum(jnp.maximum(values, -most), most).astype(held_as)


def setup_inputs(seed: int = 0) -> dict:
    key_list = jax.random.split(jax.random.key(seed), 9)
    return {
        "state": bell_draw(key_list[0], (CELLS, MEMBERS, LEV), 1.0, 6.0, ((0, 64), (1, 4))),
        "vertical_weight": bell_draw(key_list[1], (OBS, LEV), LEV ** -0.5, 0.5, ((0, 64),)),
        "horizontal_weight": jnp.clip(0.05 + 0.39999999 * jax.random.uniform(key_list[2], (OBS, NEIGH), jnp.float32) ** block_scale(key_list[2], (OBS, NEIGH), ((0, 64),), -0.2, 0.2), 0.05, 0.45),
        "obs_slot": draw_obs_slot(jax.random.fold_in(key_list[8], 71), 0),
        "request_cell": draw_request_cell(jax.random.fold_in(key_list[8], 71), 0),
        "obs_value": bell_draw(key_list[5], (OBS,), 1.0, 6.0, ((0, 64),), jnp.float32),
        "obs_error": jnp.clip(jnp.exp(math.log(2.0) - 1.3862944 * jax.random.uniform(key_list[6], (OBS,), jnp.float32) ** block_scale(key_list[6], (OBS,), ((0, 64),), -0.2, 0.2)), 0.5, 2.0),
        "obs_region": draw_obs_region(jax.random.fold_in(key_list[8], 71), 0),
    }


def reference(state, vertical_weight, horizontal_weight, obs_slot, request_cell, obs_value, obs_error, obs_region):
    halo_moves = jnp.array([-2, -1, 1, 2], dtype=jnp.int32)

    def block(src):
        slots = lax.dynamic_slice_in_dim(obs_slot, src * OBS_DEV, OBS_DEV, 0)
        table = lax.dynamic_slice_in_dim(request_cell, src, 1, 0)[0]
        within = table[slots]
        which = jnp.minimum(jnp.maximum(slots - OWN_CAP, 0) // HALO_CAP, 3).astype(jnp.int32)
        moved = jnp.mod(src + halo_moves[which], N_CELL).astype(jnp.int32)
        patch = jnp.where(slots < OWN_CAP, src, moved).astype(jnp.int32)
        cells = (patch * CELL_DEV + within).astype(jnp.int32)
        picked = state[cells].astype(jnp.float32)
        levels = lax.dynamic_slice_in_dim(vertical_weight, src * OBS_DEV, OBS_DEV, 0).astype(jnp.float32)
        column = jnp.einsum('okml,ol->okm', picked, levels)
        horiz = lax.dynamic_slice_in_dim(horizontal_weight, src * OBS_DEV, OBS_DEV, 0)
        return jnp.sum(column * horiz[:, :, None], axis=1)

    equiv = lax.map(block, jnp.arange(N_CELL, dtype=jnp.int32)).reshape(OBS, MEMBERS)
    mean = jnp.mean(equiv, axis=1, keepdims=True)
    spread = equiv - mean
    inverse = 1.0 / (obs_error * obs_error)
    innov = (obs_value - mean[:, 0]) * inverse

    def accumulate(carry, src):
        part = lax.dynamic_slice_in_dim(spread, src * OBS_DEV, OBS_DEV, 0)
        scale = lax.dynamic_slice_in_dim(inverse, src * OBS_DEV, OBS_DEV, 0)
        drive = lax.dynamic_slice_in_dim(innov, src * OBS_DEV, OBS_DEV, 0)
        region = lax.dynamic_slice_in_dim(obs_region, src * OBS_DEV, OBS_DEV, 0)
        outer = part[:, :, None] * part[:, None, :] * scale[:, None, None]
        vector = part * drive[:, None]
        total_cov = carry[0] + jax.ops.segment_sum(outer, region, num_segments=REGIONS)
        total_vec = carry[1] + jax.ops.segment_sum(vector, region, num_segments=REGIONS)
        return (total_cov, total_vec), None

    start = (jnp.zeros((REGIONS, MEMBERS, MEMBERS), jnp.float32), jnp.zeros((REGIONS, MEMBERS), jnp.float32))
    result, unused = lax.scan(accumulate, start, jnp.arange(N_CELL, dtype=jnp.int32))
    return result[0], result[1]
```

```python
import jax
import jax.numpy as jnp
from jax import lax
from jax.experimental import pallas as pl
from jax.experimental.pallas import tpu as pltpu
from jax.sharding import PartitionSpec as P

REG_DEV = 8
HALO_MOVES = (-2, -1, 1, 2)
TILE = 256
F32 = jnp.float32
BF16 = jnp.bfloat16
NT = (((1,), (1,)), ((), ()))
VMEM = pl.BlockSpec(memory_space=pltpu.VMEM)
SMEM = pl.BlockSpec(memory_space=pltpu.SMEM)


def passed_along(x, axis, by):
    devices = lax.axis_size(axis)
    return lax.ppermute(x, axis, [(i, (i + by) % devices) for i in range(devices)])


def row_stride(cells):
    return cells + 4


def slot_owner(slot_ref):
    neigh, obs = slot_ref.shape
    tops = neigh * obs // 128
    o = lax.broadcasted_iota(jnp.int32, (1, obs), 1)
    upper, lower = (o >> 5).astype(F32), (o & 31).astype(F32)
    row_top = lax.broadcasted_iota(jnp.int32, (tops, obs), 0)
    row_low = lax.broadcasted_iota(jnp.int32, (128, obs), 0)
    total = jnp.zeros((2 * tops, 128), F32)
    for k in range(neigh):
        s = slot_ref[k : k + 1, :]
        hit = row_top == (s >> 7)
        lhs = jnp.concatenate(
            [jnp.where(hit, upper, 0.0), jnp.where(hit, lower, 0.0)], axis=0
        ).astype(BF16)
        rhs = jnp.where(row_low == (s & 127), 1.0, 0.0).astype(BF16)
        total += lax.dot_general(lhs, rhs, NT, preferred_element_type=F32)
    return (32.0 * total[:tops] + total[tops:]).astype(jnp.int32)


def slot_weights(inv_ref, table_ref, vw_ref, tile):
    levels, obs = vw_ref.shape
    key = jnp.concatenate([inv_ref[2 * tile : 2 * tile + 1, :], inv_ref[2 * tile + 1 : 2 * tile + 2, :]], axis=1)
    ids = lax.broadcasted_iota(jnp.int32, (obs, TILE), 0)
    pick = jnp.where(ids == key, 1.0, 0.0).astype(BF16)
    w = jnp.dot(vw_ref[...], pick, preferred_element_type=F32)
    cells = table_ref[0:1, tile * TILE : (tile + 1) * TILE]
    sub = lax.broadcasted_iota(jnp.int32, (128 - levels, TILE), 0)
    extra = jnp.where(sub == 0, (cells >> 3).astype(F32), jnp.where(sub == 1, (cells & 7).astype(F32), 0.0))
    return jnp.concatenate([w, extra], axis=0).astype(BF16)


def ask_kernel(slot_ref, table_ref, vw_ref, inv_ref, *out_refs):
    obs = vw_ref.shape[1]
    inv_ref[...] = slot_owner(slot_ref)
    tile = obs // TILE
    for out in out_refs:
        for part in range(out.shape[1] // TILE):
            out[:, part * TILE : (part + 1) * TILE] = slot_weights(inv_ref, table_ref, vw_ref, tile)
            tile += 1


def answer_tile(cell_of, w, turned_ref, cells_dim):
    S = row_stride(cells_dim)
    half = TILE // 2
    lane = lax.broadcasted_iota(jnp.int32, (8, TILE), 1) & (half - 1)
    sub = lax.broadcasted_iota(jnp.int32, (8, 128), 0)
    wide = lax.broadcasted_iota(jnp.int32, (128, TILE), 1)
    zero = jnp.zeros_like(w)
    rhs = jnp.concatenate([jnp.where(wide < half, w, zero), jnp.where(wide < half, zero, w)], axis=0)
    first, second = [], []
    for h in range(2):
        a_rows, b_rows = [], []
        for q in range(half // 4):
            got = None
            for j in range(4):
                c = cell_of(h * half + 4 * q + j)
                a_rows.append(turned_ref[pl.ds(c, 8, stride=S), :])
                b = turned_ref[pl.ds(c + (8 - 2 * j) * S, 8, stride=S), :]
                got = b if got is None else jnp.where(sub >= 2 * j, b, got)
            b_rows.append(got)
        first.append(jnp.concatenate(a_rows, axis=0).astype(BF16))
        second.append(jnp.concatenate(b_rows, axis=0).astype(BF16))
    lhs_a = jnp.concatenate(first, axis=1)
    lhs_b = jnp.concatenate(second, axis=1)
    d_a = jnp.dot(lhs_a, rhs, preferred_element_type=F32)
    d_b = jnp.dot(lhs_b, rhs, preferred_element_type=F32)
    out_a = jnp.zeros((8, TILE), F32)
    for r in range(half):
        out_a = jnp.where(lane == r, d_a[8 * r : 8 * r + 8, :], out_a)
    out_b = jnp.zeros((8, TILE), F32)
    near = lane - (lax.broadcasted_iota(jnp.int32, (8, TILE), 0) >> 1)
    for q in range(half // 4):
        out_b = jnp.where(near == 4 * q, d_b[8 * q : 8 * q + 8, :], out_b)
    return jnp.concatenate([out_a, out_b], axis=0)


def own_kernel(state_ref, cell_ref, inv_ref, table_ref, vw_ref, turned_ref, eq_ref):
    members, levels, cells = state_ref.shape
    S = row_stride(cells)
    r = lax.broadcasted_iota(jnp.int32, (TILE, TILE), 0)
    eye = jnp.where(r == lax.broadcasted_iota(jnp.int32, (TILE, TILE), 1), 1.0, 0.0).astype(BF16)
    pad = jnp.zeros((TILE, 128 - levels), F32)
    for m in range(members):
        for part in range(cells // TILE):
            block = state_ref[m, :, part * TILE : (part + 1) * TILE]
            flat = lax.dot_general(eye, block, NT, preferred_element_type=F32)
            turned_ref[m * S + part * TILE : m * S + (part + 1) * TILE, :] = jnp.concatenate([flat, pad], axis=1)
    keep = lax.broadcasted_iota(jnp.int32, (128, TILE), 0) < levels
    for tile in range(eq_ref.shape[1] // TILE):
        w = slot_weights(inv_ref, table_ref, vw_ref, tile)
        w = jnp.where(keep, w, jnp.zeros_like(w))
        eq_ref[:, tile * TILE : (tile + 1) * TILE] = answer_tile(
            lambda i: cell_ref[0, tile * TILE + i], w, turned_ref, cells
        )


def halo_kernel(levels, cells, turned_ref, w_ref, eq_ref, words, scalars, sem):
    tail = w_ref[112:128, :].astype(F32)
    row = levels - 112
    words[...] = (8.0 * tail[row : row + 1, :] + tail[row + 1 : row + 2, :]).astype(jnp.int32)
    copy = pltpu.make_async_copy(words, scalars, sem)
    copy.start()
    copy.wait()
    keep = lax.broadcasted_iota(jnp.int32, (128, TILE), 0) < levels

    def step(tile, carry):
        at = pl.multiple_of(tile * TILE, TILE)
        w = w_ref[:, pl.ds(at, TILE)]
        w = jnp.where(keep, w, jnp.zeros_like(w))
        eq_ref[:, pl.ds(at, TILE)] = answer_tile(lambda i: scalars[0, at + i], w, turned_ref, cells)
        return carry

    lax.fori_loop(0, eq_ref.shape[1] // TILE, step, 0)


def combine_kernel(slot_ref, hw_ref, *refs):
    out_ref = refs[-1]
    neigh, obs = slot_ref.shape
    sub = lax.broadcasted_iota(jnp.int32, (8, 128), 0)
    tops, pairs = [], []
    for ref in refs[:-1]:
        for part in range(ref.shape[1] // 128):
            tops.append(ref[0:8, part * 128 : (part + 1) * 128])
            x = ref[8:16, part * 128 : (part + 1) * 128]
            x = x + pltpu.roll(x, 4, 0)
            pairs.append(x + pltpu.roll(x, 2, 0))
    quads = []
    for q in range(len(pairs) // 4):
        x = pairs[4 * q]
        for j in range(1, 4):
            x = jnp.where(sub >= 2 * j, pairs[4 * q + j], x)
        quads.append(x)
    for block in range(obs // 128):
        at = slice(block * 128, (block + 1) * 128)
        a_sum = jnp.zeros((8, 128), F32)
        b_sum = jnp.zeros((8, 128), F32)
        for k in range(neigh):
            s = jnp.broadcast_to(slot_ref[k : k + 1, at], (8, 128))
            low, top = s & 127, s >> 7
            a = jnp.zeros((8, 128), F32)
            for i, x in enumerate(tops):
                a = jnp.where(top == i, jnp.take_along_axis(x, low, axis=1, mode="promise_in_bounds"), a)
            b = jnp.zeros((8, 128), F32)
            top4 = top >> 2
            for i, x in enumerate(quads):
                b = jnp.where(top4 == i, jnp.take_along_axis(x, low, axis=1, mode="promise_in_bounds"), b)
            b = jnp.where((top & 3) == (sub >> 1), b, 0.0)
            h = hw_ref[k : k + 1, at]
            a_sum += a * h
            b_sum += b * h
        b_sum = b_sum + pltpu.roll(b_sum, 4, 0)
        b_sum = b_sum + pltpu.roll(b_sum, 2, 0)
        out_ref[0:8, at] = a_sum
        out_ref[8:16, at] = jnp.where(sub < 2, b_sum, 0.0)


def split(x):
    top = x.astype(BF16)
    return top, (x - top.astype(F32)).astype(BF16)


def cov_kernel(members, own_ref, r1_ref, r2_ref, r3_ref, value_ref, error_ref, rel_ref, mid_ref, prev_ref, next_ref):
    mem_dev = members // 4
    obs = own_ref.shape[1]
    blocks = [own_ref[...], r1_ref[...], r2_ref[...], r3_ref[...]]
    total = blocks[0] + blocks[1] + blocks[2] + blocks[3]
    mean = jnp.sum(total, axis=0, keepdims=True) * (1.0 / members)
    err = error_ref[...]
    inverse = 1.0 / (err * err)
    innov = (value_ref[...] - mean) * inverse
    row = lax.broadcasted_iota(jnp.int32, (16, obs), 0)
    spread = [jnp.where(row < mem_dev, x - mean, 0.0) for x in blocks]
    right = [x * inverse for x in spread]
    right[0] = jnp.where(row == mem_dev, innov, right[0])
    r_top, r_low = split(jnp.concatenate(right, axis=0))
    rel = rel_ref[...]
    region = lax.broadcasted_iota(jnp.int32, (REG_DEV, obs), 0)
    own = spread[0]
    own_low = own - own.astype(BF16).astype(F32)
    for g, out_ref in ((0, prev_ref), (2, next_ref), (1, mid_ref)):
        mask = rel == region + g * REG_DEV
        l_top = jnp.concatenate([jnp.where(mask, own[m : m + 1, :], 0.0) for m in range(mem_dev)], axis=0).astype(BF16)
        l_low = jnp.concatenate([jnp.where(mask, own_low[m : m + 1, :], 0.0) for m in range(mem_dev)], axis=0).astype(BF16)
        d = lax.dot_general(l_top, r_top, NT, preferred_element_type=F32)
        d += lax.dot_general(l_top, r_low, NT, preferred_element_type=F32)
        d += lax.dot_general(l_low, r_top, NT, preferred_element_type=F32)
        out_ref[...] = d


def final_kernel(mem_ref, mid_ref, a_ref, b_ref, cov_ref, proj_ref):
    mem_dev, regions, members = cov_ref.shape
    d = mid_ref[...] + a_ref[...] + b_ref[...]
    width = d.shape[1]
    i = lax.broadcasted_iota(jnp.int32, (width, members), 0)
    j = lax.broadcasted_iota(jnp.int32, (width, members), 1)
    block = (mem_ref[0] + 4 - (i >> 4)) & 3
    place = jnp.where(((i & 15) < mem_dev) & (block * mem_dev + (i & 15) == j), 1.0, 0.0)
    cov = jnp.dot(d, place, precision=lax.Precision.HIGHEST, preferred_element_type=F32)
    lane = lax.broadcasted_iota(jnp.int32, (regions, mem_dev), 1)
    proj = jnp.zeros((regions, mem_dev), F32)
    for m in range(mem_dev):
        cov_ref[m] = cov[m * regions : (m + 1) * regions, :]
        proj = jnp.where(lane == m, d[m * regions : (m + 1) * regions, mem_dev : mem_dev + 1], proj)
    proj_ref[...] = proj


def on_device(state, vertical_weight, horizontal_weight, obs_slot, request_cell, obs_value, obs_error, obs_region):
    patches = lax.axis_size("cell")
    here = lax.axis_index("cell")
    cells, mem_dev, levels = state.shape
    members = mem_dev * lax.axis_size("mem")
    obs, neigh = obs_slot.shape
    halo = 3 * obs // 4
    state_t = jnp.transpose(state, (1, 2, 0))
    vw_t, hw_t, slot_t = vertical_weight.T, horizontal_weight.T, obs_slot.T
    params = pltpu.CompilerParams(vmem_limit_bytes=40 * 1024 * 1024)

    inv, *asks = pl.pallas_call(
        ask_kernel,
        out_shape=[jax.ShapeDtypeStruct((neigh * obs // 128, 128), jnp.int32)]
        + [jax.ShapeDtypeStruct((128, halo), BF16)] * 4,
        in_specs=[VMEM] * 3,
        out_specs=[VMEM] * 5,
        compiler_params=params,
        name="ask",
    )(slot_t, request_cell, vw_t)
    arrived = [passed_along(w, "cell", by) for w, by in zip(asks, HALO_MOVES)]
    turned, eq_own = pl.pallas_call(
        own_kernel,
        out_shape=[
            jax.ShapeDtypeStruct((16 * row_stride(cells), 128), F32),
            jax.ShapeDtypeStruct((16, obs), F32),
        ],
        in_specs=[VMEM, SMEM, VMEM, VMEM, VMEM],
        out_specs=[VMEM] * 2,
        compiler_params=params,
        cost_estimate=pl.CostEstimate(flops=8_000_000_000, bytes_accessed=10_000_000, transcendentals=0),
        name="own",
    )(state_t, request_cell, inv, request_cell, vw_t)
    answer = pl.pallas_call(
        lambda *refs: halo_kernel(levels, cells, *refs),
        out_shape=jax.ShapeDtypeStruct((16, halo), F32),
        in_specs=[VMEM] * 2,
        out_specs=VMEM,
        scratch_shapes=[
            pltpu.VMEM((1, halo), jnp.int32),
            pltpu.SMEM((1, halo), jnp.int32),
            pltpu.SemaphoreType.DMA,
        ],
        compiler_params=params,
        cost_estimate=pl.CostEstimate(flops=2_000_000_000, bytes_accessed=1_000_000, transcendentals=0),
        name="answer",
    )
    back = [passed_along(answer(turned, w), "cell", -by) for w, by in zip(arrived, HALO_MOVES)]
    own = pl.pallas_call(
        combine_kernel,
        out_shape=jax.ShapeDtypeStruct((16, obs), F32),
        in_specs=[VMEM] * 7,
        out_specs=VMEM,
        compiler_params=params,
        name="combine",
    )(slot_t, hw_t, eq_own, *back)
    others = [passed_along(own, "mem", by) for by in (1, 2, 3)]
    rel = jnp.mod(obs_region - (here - 1) * REG_DEV, patches * REG_DEV)
    wide = 4 * 16
    mid, to_prev, to_next = pl.pallas_call(
        lambda *refs: cov_kernel(members, *refs),
        out_shape=[jax.ShapeDtypeStruct((mem_dev * REG_DEV, wide), F32)] * 3,
        in_specs=[VMEM] * 7,
        out_specs=[VMEM] * 3,
        compiler_params=params,
        name="cov",
    )(own, *others, obs_value.reshape(1, obs), obs_error.reshape(1, obs), rel.reshape(1, obs))
    from_prev = passed_along(to_next, "cell", 1)
    from_next = passed_along(to_prev, "cell", -1)
    cov, proj = pl.pallas_call(
        final_kernel,
        out_shape=[
            jax.ShapeDtypeStruct((mem_dev, REG_DEV, members), F32),
            jax.ShapeDtypeStruct((REG_DEV, mem_dev), F32),
        ],
        in_specs=[SMEM, VMEM, VMEM, VMEM],
        out_specs=[VMEM] * 2,
        compiler_params=params,
        name="final",
    )(lax.axis_index("mem").reshape(1).astype(jnp.int32), mid, from_prev, from_next)
    return (jnp.transpose(cov, (1, 0, 2)), proj)


def solution(mesh):
    in_specs = (
        P("cell", "mem", None),
        P("cell", None),
        P("cell", None),
        P("cell", None),
        P("cell", None),
        P("cell"),
        P("cell"),
        P("cell"),
    )
    out_specs = (P("cell", "mem", None), P("cell", "mem"))
    return jax.shard_map(
        on_device, mesh=mesh, in_specs=in_specs, out_specs=out_specs, check_vma=False
    )
```

```python
import jax
import jax.numpy as jnp
from jax import lax
from jax.experimental import pallas as pl
from jax.experimental.pallas import tpu as pltpu
from jax.sharding import PartitionSpec as P

REG_DEV = 8
HALO_MOVES = (-2, -1, 1, 2)
TILE = 256
F32 = jnp.float32
BF16 = jnp.bfloat16
NT = (((1,), (1,)), ((), ()))
VMEM = pl.BlockSpec(memory_space=pltpu.VMEM)
ANY = pl.BlockSpec(memory_space=pltpu.HBM)
SMEM = pl.BlockSpec(memory_space=pltpu.SMEM)


def passed_along(x, axis, by):
    devices = lax.axis_size(axis)
    return lax.ppermute(x, axis, [(i, (i + by) % devices) for i in range(devices)])


def row_stride(cells):
    return cells + 4


def slot_owner(slot_ref):
    neigh, obs = slot_ref.shape
    tops = neigh * obs // 128
    o = lax.broadcasted_iota(jnp.int32, (1, obs), 1)
    upper, lower = (o >> 5).astype(F32), (o & 31).astype(F32)
    row_top = lax.broadcasted_iota(jnp.int32, (tops, obs), 0)
    row_low = lax.broadcasted_iota(jnp.int32, (128, obs), 0)
    total = jnp.zeros((2 * tops, 128), F32)
    for k in range(neigh):
        s = slot_ref[k : k + 1, :]
        hit = row_top == (s >> 7)
        lhs = jnp.concatenate(
            [jnp.where(hit, upper, 0.0), jnp.where(hit, lower, 0.0)], axis=0
        ).astype(BF16)
        rhs = jnp.where(row_low == (s & 127), 1.0, 0.0).astype(BF16)
        total += lax.dot_general(lhs, rhs, NT, preferred_element_type=F32)
    return (32.0 * total[:tops] + total[tops:]).astype(jnp.int32)


def slot_weights(inv_ref, vw_ref, tile, table_ref=None):
    levels, obs = vw_ref.shape
    key = jnp.concatenate([inv_ref[2 * tile : 2 * tile + 1, :], inv_ref[2 * tile + 1 : 2 * tile + 2, :]], axis=1)
    ids = lax.broadcasted_iota(jnp.int32, (obs, TILE), 0)
    pick = jnp.where(ids == key, 1.0, 0.0).astype(BF16)
    w = jnp.dot(vw_ref[...], pick, preferred_element_type=F32)
    extra = jnp.zeros((128 - levels, TILE), F32)
    if table_ref is not None:
        cells = table_ref[0:1, tile * TILE : (tile + 1) * TILE]
        sub = lax.broadcasted_iota(jnp.int32, (128 - levels, TILE), 0)
        extra = jnp.where(sub == 0, (cells >> 3).astype(F32), jnp.where(sub == 1, (cells & 7).astype(F32), extra))
    return jnp.concatenate([w, extra], axis=0).astype(BF16)


def ask_kernel(slot_hbm, table_hbm, vw_hbm, inv_ref, vw_ref, *refs):
    *out_refs, slot_ref, table_ref, sems = refs
    copies = [
        pltpu.make_async_copy(src, dst, sems.at[i])
        for i, (src, dst) in enumerate(((slot_hbm, slot_ref), (vw_hbm, vw_ref), (table_hbm, table_ref)))
    ]
    for copy in copies:
        copy.start()
    obs = vw_ref.shape[1]
    copies[0].wait()
    inv_ref[...] = slot_owner(slot_ref)
    copies[1].wait()
    copies[2].wait()
    tile = obs // TILE
    for out in out_refs:
        for part in range(out.shape[1] // TILE):
            out[:, part * TILE : (part + 1) * TILE] = slot_weights(inv_ref, vw_ref, tile, table_ref)
            tile += 1


def answer_tile(cell_of, w, turned_ref, cells_dim):
    S = row_stride(cells_dim)
    half = TILE // 2
    lane = lax.broadcasted_iota(jnp.int32, (8, TILE), 1) & (half - 1)
    sub = lax.broadcasted_iota(jnp.int32, (8, 128), 0)
    wide = lax.broadcasted_iota(jnp.int32, (128, TILE), 1)
    zero = jnp.zeros_like(w)
    rhs = jnp.concatenate([jnp.where(wide < half, w, zero), jnp.where(wide < half, zero, w)], axis=0)
    first, second = [], []
    for h in range(2):
        a_rows, b_rows = [], []
        for q in range(half // 4):
            got = None
            for j in range(4):
                c = cell_of(h * half + 4 * q + j)
                a_rows.append(turned_ref[pl.ds(c, 8, stride=S), :])
                b = turned_ref[pl.ds(c + (8 - 2 * j) * S, 8, stride=S), :]
                got = b if got is None else jnp.where(sub >= 2 * j, b, got)
            b_rows.append(got)
        first.append(jnp.concatenate(a_rows, axis=0).astype(BF16))
        second.append(jnp.concatenate(b_rows, axis=0).astype(BF16))
    lhs_a = jnp.concatenate(first, axis=1)
    lhs_b = jnp.concatenate(second, axis=1)
    d_a = jnp.dot(lhs_a, rhs, preferred_element_type=F32)
    d_b = jnp.dot(lhs_b, rhs, preferred_element_type=F32)
    out_a = jnp.zeros((8, TILE), F32)
    for r in range(half):
        out_a = jnp.where(lane == r, d_a[8 * r : 8 * r + 8, :], out_a)
    out_b = jnp.zeros((8, TILE), F32)
    near = lane - (lax.broadcasted_iota(jnp.int32, (8, TILE), 0) >> 1)
    for q in range(half // 4):
        out_b = jnp.where(near == 4 * q, d_b[8 * q : 8 * q + 8, :], out_b)
    return jnp.concatenate([out_a, out_b], axis=0)


def own_kernel(state_hbm, table_hbm, inv_ref, vw_ref, turned_ref, eq_ref, state_ref, cell_ref, sems, cell_sem):
    members, levels, cells = state_ref.shape
    copies = [pltpu.make_async_copy(state_hbm.at[m], state_ref.at[m], sems.at[m]) for m in range(members)]
    for copy in copies:
        copy.start()
    cell_copy = pltpu.make_async_copy(table_hbm.at[:, pl.ds(0, eq_ref.shape[1])], cell_ref, cell_sem)
    cell_copy.start()
    S = row_stride(cells)
    r = lax.broadcasted_iota(jnp.int32, (TILE, TILE), 0)
    eye = jnp.where(r == lax.broadcasted_iota(jnp.int32, (TILE, TILE), 1), 1.0, 0.0).astype(BF16)
    pad = jnp.zeros((TILE, 128 - levels), F32)
    for m in range(members):
        copies[m].wait()
        for part in range(cells // TILE):
            block = state_ref[m, :, part * TILE : (part + 1) * TILE]
            flat = lax.dot_general(eye, block, NT, preferred_element_type=F32)
            turned_ref[m * S + part * TILE : m * S + (part + 1) * TILE, :] = jnp.concatenate([flat, pad], axis=1)
    cell_copy.wait()
    for tile in range(eq_ref.shape[1] // TILE):
        w = slot_weights(inv_ref, vw_ref, tile)
        eq_ref[:, tile * TILE : (tile + 1) * TILE] = answer_tile(
            lambda i: cell_ref[0, tile * TILE + i], w, turned_ref, cells
        )


def halo_kernel(levels, cells, turned_ref, w_ref, eq_ref, words, scalars, sem):
    tail = w_ref[112:128, :].astype(F32)
    row = levels - 112
    words[...] = (8.0 * tail[row : row + 1, :] + tail[row + 1 : row + 2, :]).astype(jnp.int32)
    copy = pltpu.make_async_copy(words, scalars, sem)
    copy.start()
    copy.wait()
    keep = lax.broadcasted_iota(jnp.int32, (128, TILE), 0) < levels

    def step(tile, carry):
        at = pl.multiple_of(tile * TILE, TILE)
        w = w_ref[:, pl.ds(at, TILE)]
        w = jnp.where(keep, w, jnp.zeros_like(w))
        eq_ref[:, pl.ds(at, TILE)] = answer_tile(lambda i: scalars[0, at + i], w, turned_ref, cells)
        return carry

    lax.fori_loop(0, eq_ref.shape[1] // TILE, step, 0)


def combine_kernel(slot_ref, hw_ref, *refs):
    out_ref = refs[-1]
    neigh, obs = slot_ref.shape
    sub = lax.broadcasted_iota(jnp.int32, (8, 128), 0)
    tops, pairs = [], []
    for ref in refs[:-1]:
        for part in range(ref.shape[1] // 128):
            tops.append(ref[0:8, part * 128 : (part + 1) * 128])
            x = ref[8:16, part * 128 : (part + 1) * 128]
            x = x + pltpu.roll(x, 4, 0)
            pairs.append(x + pltpu.roll(x, 2, 0))
    quads = []
    for q in range(len(pairs) // 4):
        x = pairs[4 * q]
        for j in range(1, 4):
            x = jnp.where(sub >= 2 * j, pairs[4 * q + j], x)
        quads.append(x)
    for block in range(obs // 128):
        at = slice(block * 128, (block + 1) * 128)
        a_sum = jnp.zeros((8, 128), F32)
        b_sum = jnp.zeros((8, 128), F32)
        for k in range(neigh):
            s = jnp.broadcast_to(slot_ref[k : k + 1, at], (8, 128))
            low, top = s & 127, s >> 7
            a = jnp.zeros((8, 128), F32)
            for i, x in enumerate(tops):
                a = jnp.where(top == i, jnp.take_along_axis(x, low, axis=1, mode="promise_in_bounds"), a)
            b = jnp.zeros((8, 128), F32)
            top4 = top >> 2
            for i, x in enumerate(quads):
                b = jnp.where(top4 == i, jnp.take_along_axis(x, low, axis=1, mode="promise_in_bounds"), b)
            b = jnp.where((top & 3) == (sub >> 1), b, 0.0)
            h = hw_ref[k : k + 1, at]
            a_sum += a * h
            b_sum += b * h
        b_sum = b_sum + pltpu.roll(b_sum, 4, 0)
        b_sum = b_sum + pltpu.roll(b_sum, 2, 0)
        out_ref[0:8, at] = a_sum
        out_ref[8:16, at] = jnp.where(sub < 2, b_sum, 0.0)


def split(x):
    top = x.astype(BF16)
    return top, (x - top.astype(F32)).astype(BF16)


def cov_kernel(members, own_ref, r1_ref, r2_ref, r3_ref, value_ref, error_ref, rel_ref, mid_ref, prev_ref, next_ref):
    mem_dev = members // 4
    obs = own_ref.shape[1]
    blocks = [own_ref[...], r1_ref[...], r2_ref[...], r3_ref[...]]
    total = blocks[0] + blocks[1] + blocks[2] + blocks[3]
    mean = jnp.sum(total, axis=0, keepdims=True) * (1.0 / members)
    err = error_ref[...]
    inverse = 1.0 / (err * err)
    innov = (value_ref[...] - mean) * inverse
    row = lax.broadcasted_iota(jnp.int32, (16, obs), 0)
    spread = [jnp.where(row < mem_dev, x - mean, 0.0) for x in blocks]
    right = [x * inverse for x in spread]
    right[0] = jnp.where(row == mem_dev, innov, right[0])
    r_top, r_low = split(jnp.concatenate(right, axis=0))
    rel = rel_ref[...]
    region = lax.broadcasted_iota(jnp.int32, (REG_DEV, obs), 0)
    own = spread[0]
    own_low = own - own.astype(BF16).astype(F32)
    for g, out_ref in ((0, prev_ref), (2, next_ref), (1, mid_ref)):
        mask = rel == region + g * REG_DEV
        l_top = jnp.concatenate([jnp.where(mask, own[m : m + 1, :], 0.0) for m in range(mem_dev)], axis=0).astype(BF16)
        l_low = jnp.concatenate([jnp.where(mask, own_low[m : m + 1, :], 0.0) for m in range(mem_dev)], axis=0).astype(BF16)
        d = lax.dot_general(l_top, r_top, NT, preferred_element_type=F32)
        d += lax.dot_general(l_top, r_low, NT, preferred_element_type=F32)
        d += lax.dot_general(l_low, r_top, NT, preferred_element_type=F32)
        out_ref[...] = d


def final_kernel(mem_ref, mid_ref, a_ref, b_ref, cov_ref, proj_ref):
    mem_dev, regions, members = cov_ref.shape
    d = mid_ref[...] + a_ref[...] + b_ref[...]
    width = d.shape[1]
    i = lax.broadcasted_iota(jnp.int32, (width, members), 0)
    j = lax.broadcasted_iota(jnp.int32, (width, members), 1)
    block = (mem_ref[0] + 4 - (i >> 4)) & 3
    place = jnp.where(((i & 15) < mem_dev) & (block * mem_dev + (i & 15) == j), 1.0, 0.0)
    cov = jnp.dot(d, place, precision=lax.Precision.HIGHEST, preferred_element_type=F32)
    lane = lax.broadcasted_iota(jnp.int32, (regions, mem_dev), 1)
    proj = jnp.zeros((regions, mem_dev), F32)
    for m in range(mem_dev):
        cov_ref[m] = cov[m * regions : (m + 1) * regions, :]
        proj = jnp.where(lane == m, d[m * regions : (m + 1) * regions, mem_dev : mem_dev + 1], proj)
    proj_ref[...] = proj


def on_device(state, vertical_weight, horizontal_weight, obs_slot, request_cell, obs_value, obs_error, obs_region):
    patches = lax.axis_size("cell")
    here = lax.axis_index("cell")
    cells, mem_dev, levels = state.shape
    members = mem_dev * lax.axis_size("mem")
    obs, neigh = obs_slot.shape
    halo = 3 * obs // 4
    state_t = jnp.transpose(state, (1, 2, 0))
    vw_t, hw_t, slot_t = vertical_weight.T, horizontal_weight.T, obs_slot.T
    far = lambda x: pltpu.with_memory_space_constraint(x, pltpu.HBM)
    params = pltpu.CompilerParams(vmem_limit_bytes=16 * 1024 * 1024)

    inv, vw_near, *asks = pl.pallas_call(
        ask_kernel,
        out_shape=[
            jax.ShapeDtypeStruct((neigh * obs // 128, 128), jnp.int32),
            jax.ShapeDtypeStruct((levels, obs), BF16),
        ]
        + [jax.ShapeDtypeStruct((128, halo), BF16)] * 4,
        in_specs=[ANY] * 3,
        out_specs=[VMEM] * 6,
        scratch_shapes=[
            pltpu.VMEM((neigh, obs), jnp.int32),
            pltpu.VMEM((1, neigh * obs), jnp.int32),
            pltpu.SemaphoreType.DMA((3,)),
        ],
        compiler_params=params,
        name="ask",
    )(far(slot_t), far(request_cell), far(vw_t))
    arrived = [passed_along(w, "cell", by) for w, by in zip(asks, HALO_MOVES)]
    turned, eq_own = pl.pallas_call(
        own_kernel,
        out_shape=[
            pltpu.VMEM((16 * row_stride(cells), 128), F32),
            jax.ShapeDtypeStruct((16, obs), F32),
        ],
        in_specs=[ANY, ANY, VMEM, VMEM],
        out_specs=[VMEM] * 2,
        scratch_shapes=[
            pltpu.VMEM((mem_dev, levels, cells), BF16),
            pltpu.SMEM((1, obs), jnp.int32),
            pltpu.SemaphoreType.DMA((mem_dev,)),
            pltpu.SemaphoreType.DMA,
        ],
        compiler_params=params,
        cost_estimate=pl.CostEstimate(flops=8_000_000_000, bytes_accessed=10_000_000, transcendentals=0),
        name="own",
    )(far(state_t), far(request_cell), inv, vw_near)
    answer = pl.pallas_call(
        lambda *refs: halo_kernel(levels, cells, *refs),
        out_shape=jax.ShapeDtypeStruct((16, halo), F32),
        in_specs=[VMEM] * 2,
        out_specs=VMEM,
        scratch_shapes=[
            pltpu.VMEM((1, halo), jnp.int32),
            pltpu.SMEM((1, halo), jnp.int32),
            pltpu.SemaphoreType.DMA,
        ],
        compiler_params=params,
        cost_estimate=pl.CostEstimate(flops=2_000_000_000, bytes_accessed=1_000_000, transcendentals=0),
        name="answer",
    )
    back = [passed_along(answer(turned, w), "cell", -by) for w, by in zip(arrived, HALO_MOVES)]
    own = pl.pallas_call(
        combine_kernel,
        out_shape=jax.ShapeDtypeStruct((16, obs), F32),
        in_specs=[VMEM] * 7,
        out_specs=VMEM,
        compiler_params=params,
        name="combine",
    )(slot_t, hw_t, eq_own, *back)
    others = [passed_along(own, "mem", by) for by in (1, 2, 3)]
    rel = jnp.mod(obs_region - (here - 1) * REG_DEV, patches * REG_DEV)
    wide = 4 * 16
    mid, to_prev, to_next = pl.pallas_call(
        lambda *refs: cov_kernel(members, *refs),
        out_shape=[jax.ShapeDtypeStruct((mem_dev * REG_DEV, wide), F32)] * 3,
        in_specs=[VMEM] * 7,
        out_specs=[VMEM] * 3,
        compiler_params=params,
        name="cov",
    )(own, *others, obs_value.reshape(1, obs), obs_error.reshape(1, obs), rel.reshape(1, obs))
    from_prev = passed_along(to_next, "cell", 1)
    from_next = passed_along(to_prev, "cell", -1)
    cov, proj = pl.pallas_call(
        final_kernel,
        out_shape=[
            jax.ShapeDtypeStruct((mem_dev, REG_DEV, members), F32),
            jax.ShapeDtypeStruct((REG_DEV, mem_dev), F32),
        ],
        in_specs=[SMEM, VMEM, VMEM, VMEM],
        out_specs=[VMEM] * 2,
        compiler_params=params,
        name="final",
    )(lax.axis_index("mem").reshape(1).astype(jnp.int32), mid, from_prev, from_next)
    return (jnp.transpose(cov, (1, 0, 2)), proj)


def solution(mesh):
    in_specs = (
        P("cell", "mem", None),
        P("cell", None),
        P("cell", None),
        P("cell", None),
        P("cell", None),
        P("cell"),
        P("cell"),
        P("cell"),
    )
    out_specs = (P("cell", "mem", None), P("cell", "mem"))
    return jax.shard_map(
        on_device, mesh=mesh, in_specs=in_specs, out_specs=out_specs, check_vma=False
    )
```

```python
import jax
import jax.numpy as jnp
from jax import lax
from jax.experimental import pallas as pl
from jax.experimental.pallas import tpu as pltpu
from jax.sharding import PartitionSpec as P

REG_DEV = 8
HALO_MOVES = (-2, -1, 1, 2)
TILE = 256
F32 = jnp.float32
BF16 = jnp.bfloat16
NT = (((1,), (1,)), ((), ()))
VMEM = pl.BlockSpec(memory_space=pltpu.VMEM)
ANY = pl.BlockSpec(memory_space=pltpu.HBM)
SMEM = pl.BlockSpec(memory_space=pltpu.SMEM)


def passed_along(x, axis, by):
    devices = lax.axis_size(axis)
    return lax.ppermute(x, axis, [(i, (i + by) % devices) for i in range(devices)])


def row_stride(cells):
    return cells + 4


def member_row(cells, m):
    return m * row_stride(cells) + (m >= 8)


def slot_owner(slot_ref):
    neigh, obs = slot_ref.shape
    tops = neigh * obs // 128
    o = lax.broadcasted_iota(jnp.int32, (1, obs), 1)
    upper, lower = (o >> 5).astype(F32), (o & 31).astype(F32)
    row_top = lax.broadcasted_iota(jnp.int32, (tops, obs), 0)
    row_low = lax.broadcasted_iota(jnp.int32, (128, obs), 0)
    total = jnp.zeros((2 * tops, 128), F32)
    for k in range(neigh):
        s = slot_ref[k : k + 1, :]
        hit = row_top == (s >> 7)
        lhs = jnp.concatenate(
            [jnp.where(hit, upper, 0.0), jnp.where(hit, lower, 0.0)], axis=0
        ).astype(BF16)
        rhs = jnp.where(row_low == (s & 127), 1.0, 0.0).astype(BF16)
        total += lax.dot_general(lhs, rhs, NT, preferred_element_type=F32)
    return (32.0 * total[:tops] + total[tops:]).astype(jnp.int32)


def slot_weights(inv_ref, vw_ref, tile, table_ref=None):
    levels, obs = vw_ref.shape
    key = jnp.concatenate([inv_ref[2 * tile : 2 * tile + 1, :], inv_ref[2 * tile + 1 : 2 * tile + 2, :]], axis=1)
    ids = lax.broadcasted_iota(jnp.int32, (obs, TILE), 0)
    pick = jnp.where(ids == key, 1.0, 0.0).astype(BF16)
    w = jnp.dot(vw_ref[...], pick, preferred_element_type=F32)
    extra = jnp.zeros((128 - levels, TILE), F32)
    if table_ref is not None:
        cells = table_ref[0:1, tile * TILE : (tile + 1) * TILE]
        sub = lax.broadcasted_iota(jnp.int32, (128 - levels, TILE), 0)
        extra = jnp.where(sub == 0, (cells >> 3).astype(F32), jnp.where(sub == 1, (cells & 7).astype(F32), extra))
    return jnp.concatenate([w, extra], axis=0).astype(BF16)


def ask_far_kernel(slot_hbm, table_hbm, vw_hbm, state_hbm, inv_ref, vw_ref, table_ref, state_ref, *refs):
    *out_refs, slot_ref, sems = refs
    members, levels, cells = state_hbm.shape
    pairs = (
        (slot_hbm, slot_ref),
        (vw_hbm, vw_ref),
        (table_hbm, table_ref),
        (state_hbm, state_ref.at[:, pl.ds(0, levels), :]),
    )
    copies = [pltpu.make_async_copy(src, dst, sems.at[i]) for i, (src, dst) in enumerate(pairs)]
    for copy in copies:
        copy.start()
    copies[0].wait()
    inv_ref[...] = slot_owner(slot_ref)
    copies[1].wait()
    copies[2].wait()
    halo_weights(inv_ref, vw_ref, table_ref, out_refs, (0, 3))
    copies[3].wait()
    for m in range(members):
        state_ref[m, levels:, :] = jnp.zeros((state_ref.shape[1] - levels, cells), BF16)


def ask_near_kernel(inv_ref, vw_ref, table_ref, own_ref, *out_refs):
    halo_weights(inv_ref, vw_ref, table_ref, out_refs, (1, 2))
    for tile in range(own_ref.shape[1] // TILE):
        own_ref[:, tile * TILE : (tile + 1) * TILE] = slot_weights(inv_ref, vw_ref, tile)


def halo_weights(inv_ref, vw_ref, table_ref, out_refs, numbers):
    obs = vw_ref.shape[1]
    for out, number in zip(out_refs, numbers):
        count = out.shape[1] // TILE
        for part in range(count):
            tile = obs // TILE + number * count + part
            out[:, part * TILE : (part + 1) * TILE] = slot_weights(inv_ref, vw_ref, tile, table_ref)


def answer_tile(cell_of, w, turned_ref, cells_dim):
    S, rest = row_stride(cells_dim), member_row(cells_dim, 8)
    half = TILE // 2
    lane = lax.broadcasted_iota(jnp.int32, (8, TILE), 1) & (half - 1)
    wide = lax.broadcasted_iota(jnp.int32, (128, TILE), 1)
    zero = jnp.zeros_like(w)
    rhs = jnp.concatenate([jnp.where(wide < half, w, zero), jnp.where(wide < half, zero, w)], axis=0)
    first, second = [], []
    for h in range(2):
        a_rows, b_rows = [], []
        for q in range(half // 4):
            for j in range(4):
                c = cell_of(h * half + 4 * q + j)
                a_rows.append(turned_ref[pl.ds(c, 8, stride=S), :])
                b_rows.append(turned_ref[pl.ds(c + rest, 2, stride=S), :])
        first.append(jnp.concatenate(a_rows, axis=0).astype(BF16))
        second.append(jnp.concatenate(b_rows, axis=0).astype(BF16))
    lhs_a = jnp.concatenate(first, axis=1)
    lhs_b = jnp.concatenate(second, axis=1)
    d_a = jnp.dot(lhs_a, rhs, preferred_element_type=F32)
    d_b = jnp.dot(lhs_b, rhs, preferred_element_type=F32)
    out_a = jnp.zeros((8, TILE), F32)
    for r in range(half):
        out_a = jnp.where(lane == r, d_a[8 * r : 8 * r + 8, :], out_a)
    out_b = jnp.zeros((8, TILE), F32)
    near = lane - (lax.broadcasted_iota(jnp.int32, (8, TILE), 0) >> 1)
    for q in range(half // 4):
        out_b = jnp.where(near == 4 * q, d_b[8 * q : 8 * q + 8, :], out_b)
    return jnp.concatenate([out_a, out_b], axis=0)


def own_kernel(state_ref, table_hbm, w_ref, turned_ref, eq_ref, cell_ref, cell_sem):
    members, levels, cells = state_ref.shape
    copy = pltpu.make_async_copy(table_hbm.at[:, pl.ds(0, eq_ref.shape[1])], cell_ref, cell_sem)
    copy.start()
    r = lax.broadcasted_iota(jnp.int32, (TILE, TILE), 0)
    eye = jnp.where(r == lax.broadcasted_iota(jnp.int32, (TILE, TILE), 1), 1.0, 0.0).astype(BF16)
    for m in range(0, members, 2):
        for part in range(cells // TILE):
            at = slice(part * TILE, (part + 1) * TILE)
            block = jnp.concatenate([state_ref[m, :, at], state_ref[m + 1, :, at]], axis=0)
            flat = lax.dot_general(eye, block, NT, preferred_element_type=F32)
            for i in range(2):
                low = member_row(cells, m + i) + part * TILE
                turned_ref[low : low + TILE, :] = flat[:, i * 128 : (i + 1) * 128]
    copy.wait()
    for tile in range(eq_ref.shape[1] // TILE):
        at = slice(tile * TILE, (tile + 1) * TILE)
        eq_ref[:, at] = answer_tile(lambda i: cell_ref[0, tile * TILE + i], w_ref[:, at], turned_ref, cells)


def answer_kernel(levels, cells, turned_ref, *refs):
    count = len(refs) // 4
    w_refs, eq_refs = refs[:count], refs[count : 2 * count]
    words, scalars, sems = refs[2 * count : 3 * count], refs[3 * count : 4 * count], refs[-1]
    copies = []
    for i in range(count):
        tail = w_refs[i][112:128, :].astype(F32)
        row = levels - 112
        words[i][...] = (8.0 * tail[row : row + 1, :] + tail[row + 1 : row + 2, :]).astype(jnp.int32)
        copies.append(pltpu.make_async_copy(words[i], scalars[i], sems.at[i]))
        copies[-1].start()
    keep = lax.broadcasted_iota(jnp.int32, (128, TILE), 0) < levels
    for copy in copies:
        copy.wait()
    for i in range(count):
        for tile in range(eq_refs[i].shape[1] // TILE):
            at = slice(tile * TILE, (tile + 1) * TILE)
            w = w_refs[i][:, at]
            w = jnp.where(keep, w, jnp.zeros_like(w))
            eq_refs[i][:, at] = answer_tile(lambda j: scalars[i][0, tile * TILE + j], w, turned_ref, cells)


def combine_kernel(firsts, slot_ref, hw_ref, *refs):
    *eq_refs, out_ref = refs
    before = eq_refs.pop(0) if len(eq_refs) > len(firsts) else None
    neigh, obs = slot_ref.shape
    sub = lax.broadcasted_iota(jnp.int32, (8, 128), 0)
    tops, pairs = {}, {}
    for first, ref in zip(firsts, eq_refs):
        for part in range(ref.shape[1] // 128):
            tops[first + part] = ref[0:8, part * 128 : (part + 1) * 128]
            x = ref[8:16, part * 128 : (part + 1) * 128]
            x = x + pltpu.roll(x, 4, 0)
            pairs[first + part] = x + pltpu.roll(x, 2, 0)
    quads = {}
    for q in sorted({i // 4 for i in pairs}):
        x = jnp.zeros((8, 128), F32)
        for j in range(4):
            if 4 * q + j in pairs:
                x = jnp.where(sub >> 1 == j, pairs[4 * q + j], x)
        quads[q] = x
    last = None
    for block in range(obs // 128):
        at = slice(block * 128, (block + 1) * 128)
        a_sum = jnp.zeros((8, 128), F32)
        b_sum = jnp.zeros((8, 128), F32)
        for k in range(neigh):
            s = jnp.broadcast_to(slot_ref[k : k + 1, at], (8, 128))
            low, top = s & 127, s >> 7
            a = jnp.zeros((8, 128), F32)
            for i, x in tops.items():
                a = jnp.where(top == i, jnp.take_along_axis(x, low, axis=1, mode="promise_in_bounds"), a)
            b = jnp.zeros((8, 128), F32)
            top4 = top >> 2
            for i, x in quads.items():
                b = jnp.where(top4 == i, jnp.take_along_axis(x, low, axis=1, mode="promise_in_bounds"), b)
            b = jnp.where((top & 3) == (sub >> 1), b, 0.0)
            h = hw_ref[k : k + 1, at]
            a_sum += a * h
            b_sum += b * h
        b_sum = b_sum + pltpu.roll(b_sum, 4, 0)
        b_sum = b_sum + pltpu.roll(b_sum, 2, 0)
        if before is not None:
            a_sum += before[:, at]
        out_ref[:, at] = a_sum
        last = b_sum if block % 4 == 0 else jnp.where(sub >> 1 >= block % 4, b_sum, last)
        if block % 4 == 3:
            low = obs + block // 4 * 128
            if before is not None:
                last += before[:, low : low + 128]
            out_ref[:, low : low + 128] = last


def unpacked(ref, obs):
    sub = lax.broadcasted_iota(jnp.int32, (8, 128), 0)
    rest = []
    for block in range(obs // 128):
        low = obs + block // 4 * 128
        x = ref[:, low : low + 128]
        if block % 4:
            x = pltpu.roll(x, 8 - 2 * (block % 4), 0)
        rest.append(jnp.where(sub < 2, x, 0.0))
    return jnp.concatenate([ref[:, :obs], jnp.concatenate(rest, axis=1)], axis=0)


def split(x):
    top = x.astype(BF16)
    return top, (x - top.astype(F32)).astype(BF16)


def cov_kernel(members, own_ref, r1_ref, r2_ref, r3_ref, value_ref, error_ref, region_ref, mid_ref, prev_ref, next_ref):
    mem_dev = members // 4
    obs = region_ref.shape[1]
    blocks = [unpacked(ref, obs) for ref in (own_ref, r1_ref, r2_ref, r3_ref)]
    total = blocks[0] + blocks[1] + blocks[2] + blocks[3]
    mean = jnp.sum(total, axis=0, keepdims=True) * (1.0 / members)
    err = error_ref[...]
    inverse = 1.0 / (err * err)
    innov = (value_ref[...] - mean) * inverse
    row = lax.broadcasted_iota(jnp.int32, (16, obs), 0)
    spread = [jnp.where(row < mem_dev, x - mean, 0.0) for x in blocks]
    right = [x * inverse for x in spread]
    right[0] = jnp.where(row == mem_dev, innov, right[0])
    r_top, r_low = split(jnp.concatenate(right, axis=0))
    regions = lax.axis_size("cell") * REG_DEV
    rel = region_ref[...] - (lax.axis_index("cell") - 1) * REG_DEV
    rel = jnp.where(rel < 0, rel + regions, rel)
    rel = jnp.where(rel >= regions, rel - regions, rel)
    region = lax.broadcasted_iota(jnp.int32, (REG_DEV, obs), 0)
    own = spread[0]
    own_low = own - own.astype(BF16).astype(F32)
    for g, out_ref in ((0, prev_ref), (2, next_ref), (1, mid_ref)):
        mask = rel == region + g * REG_DEV
        l_top = jnp.concatenate([jnp.where(mask, own[m : m + 1, :], 0.0) for m in range(mem_dev)], axis=0).astype(BF16)
        l_low = jnp.concatenate([jnp.where(mask, own_low[m : m + 1, :], 0.0) for m in range(mem_dev)], axis=0).astype(BF16)
        d = lax.dot_general(l_top, r_top, NT, preferred_element_type=F32)
        d += lax.dot_general(l_top, r_low, NT, preferred_element_type=F32)
        d += lax.dot_general(l_low, r_top, NT, preferred_element_type=F32)
        out_ref[...] = d


def final_kernel(mid_ref, a_ref, b_ref, cov_ref, proj_ref):
    mem_dev, regions, members = cov_ref.shape
    d = mid_ref[...] + a_ref[...] + b_ref[...]
    width = d.shape[1]
    i = lax.broadcasted_iota(jnp.int32, (width, members), 0)
    j = lax.broadcasted_iota(jnp.int32, (width, members), 1)
    block = (lax.axis_index("mem") + 4 - (i >> 4)) & 3
    place = jnp.where(((i & 15) < mem_dev) & (block * mem_dev + (i & 15) == j), 1.0, 0.0)
    cov = jnp.dot(d, place, precision=lax.Precision.HIGHEST, preferred_element_type=F32)
    lane = lax.broadcasted_iota(jnp.int32, (regions, mem_dev), 1)
    proj = jnp.zeros((regions, mem_dev), F32)
    for m in range(mem_dev):
        cov_ref[m] = cov[m * regions : (m + 1) * regions, :]
        proj = jnp.where(lane == m, d[m * regions : (m + 1) * regions, mem_dev : mem_dev + 1], proj)
    proj_ref[...] = proj


def on_device(state, vertical_weight, horizontal_weight, obs_slot, request_cell, obs_value, obs_error, obs_region):
    cells, mem_dev, levels = state.shape
    members = mem_dev * lax.axis_size("mem")
    obs, neigh = obs_slot.shape
    halo = 3 * obs // 4
    state_t = jnp.transpose(state, (1, 2, 0))
    vw_t, hw_t, slot_t = vertical_weight.T, horizontal_weight.T, obs_slot.T
    far = lambda x: pltpu.with_memory_space_constraint(x, pltpu.HBM)
    params = pltpu.CompilerParams(vmem_limit_bytes=16 * 1024 * 1024)

    w_shape = jax.ShapeDtypeStruct((128, halo), BF16)
    inv, vw_near, table, state_near, ask_m2, ask_p2 = pl.pallas_call(
        ask_far_kernel,
        out_shape=[
            pltpu.VMEM((neigh * obs // 128, 128), jnp.int32),
            pltpu.VMEM((levels, obs), BF16),
            pltpu.VMEM((1, neigh * obs), jnp.int32),
            pltpu.VMEM((mem_dev, 128, cells), BF16),
            w_shape,
            w_shape,
        ],
        in_specs=[ANY] * 4,
        out_specs=[VMEM] * 6,
        scratch_shapes=[pltpu.VMEM((neigh, obs), jnp.int32), pltpu.SemaphoreType.DMA((4,))],
        compiler_params=params,
        cost_estimate=pl.CostEstimate(flops=2_000_000_000, bytes_accessed=6_000_000, transcendentals=0),
        name="ask_far",
    )(far(slot_t), far(request_cell), far(vw_t), far(state_t))
    w_m2, w_p2 = passed_along(ask_m2, "cell", -2), passed_along(ask_p2, "cell", 2)
    w_own, ask_m1, ask_p1 = pl.pallas_call(
        ask_near_kernel,
        out_shape=[pltpu.VMEM((128, obs), BF16), w_shape, w_shape],
        in_specs=[VMEM] * 3,
        out_specs=[VMEM] * 3,
        compiler_params=params,
        cost_estimate=pl.CostEstimate(flops=2_000_000_000, bytes_accessed=1_000_000, transcendentals=0),
        name="ask_near",
    )(inv, vw_near, table)
    w_m1, w_p1 = passed_along(ask_m1, "cell", -1), passed_along(ask_p1, "cell", 1)
    turned, eq_own = pl.pallas_call(
        own_kernel,
        out_shape=[
            pltpu.VMEM((mem_dev * row_stride(cells), 128), F32),
            pltpu.VMEM((16, obs), F32),
        ],
        in_specs=[VMEM, ANY, VMEM],
        out_specs=[VMEM] * 2,
        scratch_shapes=[pltpu.SMEM((1, obs), jnp.int32), pltpu.SemaphoreType.DMA],
        compiler_params=params,
        cost_estimate=pl.CostEstimate(flops=8_000_000_000, bytes_accessed=10_000_000, transcendentals=0),
        name="own",
    )(state_near, far(request_cell), w_own)
    turned = pltpu.with_memory_space_constraint(turned, pltpu.VMEM)
    answer = pl.pallas_call(
        lambda *refs: answer_kernel(levels, cells, *refs),
        out_shape=[jax.ShapeDtypeStruct((16, halo), F32)] * 2,
        in_specs=[VMEM] * 3,
        out_specs=[VMEM] * 2,
        scratch_shapes=[pltpu.VMEM((1, halo), jnp.int32)] * 2
        + [pltpu.SMEM((1, halo), jnp.int32)] * 2
        + [pltpu.SemaphoreType.DMA((2,))],
        compiler_params=params,
        cost_estimate=pl.CostEstimate(flops=4_000_000_000, bytes_accessed=1_000_000, transcendentals=0),
        name="answer",
    )
    eq_m2, eq_p2 = answer(turned, w_m2, w_p2)
    eq_m2, eq_p2 = passed_along(eq_m2, "cell", 2), passed_along(eq_p2, "cell", -2)
    eq_m1, eq_p1 = answer(turned, w_m1, w_p1)
    eq_m1, eq_p1 = passed_along(eq_m1, "cell", 1), passed_along(eq_p1, "cell", -1)

    def combine(tables, *before):
        firsts = [obs // 128 + n * halo // 128 if n >= 0 else 0 for n, _ in tables]
        return pl.pallas_call(
            lambda *refs: combine_kernel(firsts, *refs),
            out_shape=jax.ShapeDtypeStruct((8, obs + obs // 4), F32),
            in_specs=[VMEM] * (2 + len(before) + len(tables)),
            out_specs=VMEM,
            compiler_params=params,
            cost_estimate=pl.CostEstimate(flops=1_000_000_000, bytes_accessed=1_000_000, transcendentals=0),
            name="combine",
        )(slot_t, hw_t, *before, *(x for _, x in tables))

    own = combine([(-1, eq_own), (0, eq_m2), (3, eq_p2)])
    own = combine([(1, eq_m1), (2, eq_p1)], own)
    others = [passed_along(own, "mem", by) for by in (1, 2, 3)]
    wide = 4 * 16
    mid, to_prev, to_next = pl.pallas_call(
        lambda *refs: cov_kernel(members, *refs),
        out_shape=[jax.ShapeDtypeStruct((mem_dev * REG_DEV, wide), F32)] * 3,
        in_specs=[VMEM] * 7,
        out_specs=[VMEM] * 3,
        compiler_params=params,
        name="cov",
    )(own, *others, obs_value.reshape(1, obs), obs_error.reshape(1, obs), obs_region.reshape(1, obs))
    from_prev = passed_along(to_next, "cell", 1)
    from_next = passed_along(to_prev, "cell", -1)
    cov, proj = pl.pallas_call(
        final_kernel,
        out_shape=[
            jax.ShapeDtypeStruct((mem_dev, REG_DEV, members), F32),
            jax.ShapeDtypeStruct((REG_DEV, mem_dev), F32),
        ],
        in_specs=[VMEM] * 3,
        out_specs=[VMEM] * 2,
        compiler_params=params,
        name="final",
    )(mid, from_prev, from_next)
    return (jnp.transpose(cov, (1, 0, 2)), proj)


def solution(mesh):
    in_specs = (
        P("cell", "mem", None),
        P("cell", None),
        P("cell", None),
        P("cell", None),
        P("cell", None),
        P("cell"),
        P("cell"),
        P("cell"),
    )
    out_specs = (P("cell", "mem", None), P("cell", "mem"))
    return jax.shard_map(
        on_device, mesh=mesh, in_specs=in_specs, out_specs=out_specs, check_vma=False
    )
```

```python
import jax
import jax.numpy as jnp
from jax import lax
from jax.experimental import pallas as pl
from jax.experimental.pallas import tpu as pltpu
from jax.sharding import PartitionSpec as P

REG_DEV = 8
HALO_MOVES = (-2, -1, 1, 2)
TILE = 256
F32 = jnp.float32
BF16 = jnp.bfloat16
NT = (((1,), (1,)), ((), ()))
VMEM = pl.BlockSpec(memory_space=pltpu.VMEM)
ANY = pl.BlockSpec(memory_space=pltpu.HBM)
SMEM = pl.BlockSpec(memory_space=pltpu.SMEM)


def passed_along(x, axis, by):
    devices = lax.axis_size(axis)
    return lax.ppermute(x, axis, [(i, (i + by) % devices) for i in range(devices)])


def row_stride(cells):
    return cells + 4


def member_row(cells, m):
    return m * row_stride(cells) + (m >= 8)


def slot_owner(slot_ref):
    neigh, obs = slot_ref.shape
    tops = neigh * obs // 128
    o = lax.broadcasted_iota(jnp.int32, (1, obs), 1)
    upper, lower = (o >> 5).astype(F32), (o & 31).astype(F32)
    row_top = lax.broadcasted_iota(jnp.int32, (tops, obs), 0)
    row_low = lax.broadcasted_iota(jnp.int32, (128, obs), 0)
    total = jnp.zeros((2 * tops, 128), F32)
    for k in range(neigh):
        s = slot_ref[k : k + 1, :]
        hit = row_top == (s >> 7)
        lhs = jnp.concatenate(
            [jnp.where(hit, upper, 0.0), jnp.where(hit, lower, 0.0)], axis=0
        ).astype(BF16)
        rhs = jnp.where(row_low == (s & 127), 1.0, 0.0).astype(BF16)
        total += lax.dot_general(lhs, rhs, NT, preferred_element_type=F32)
    return (32.0 * total[:tops] + total[tops:]).astype(jnp.int32)


def slot_weights(inv_ref, vw_ref, tile, table_ref=None):
    levels, obs = vw_ref.shape
    key = jnp.concatenate([inv_ref[2 * tile : 2 * tile + 1, :], inv_ref[2 * tile + 1 : 2 * tile + 2, :]], axis=1)
    ids = lax.broadcasted_iota(jnp.int32, (obs, TILE), 0)
    pick = jnp.where(ids == key, 1.0, 0.0).astype(BF16)
    w = jnp.dot(vw_ref[...], pick, preferred_element_type=F32)
    extra = jnp.zeros((128 - levels, TILE), F32)
    if table_ref is not None:
        cells = table_ref[0:1, tile * TILE : (tile + 1) * TILE]
        sub = lax.broadcasted_iota(jnp.int32, (128 - levels, TILE), 0)
        extra = jnp.where(sub == 0, (cells >> 3).astype(F32), jnp.where(sub == 1, (cells & 7).astype(F32), extra))
    return jnp.concatenate([w, extra], axis=0).astype(BF16)


def ask_low_kernel(slot_hbm, table_hbm, vw_hbm, state_hbm, inv_ref, vw_ref, table_ref, state_ref, *refs):
    *out_refs, slot_ref, sems = refs
    members, levels, cells = state_hbm.shape
    pairs = (
        (slot_hbm, slot_ref),
        (vw_hbm, vw_ref),
        (table_hbm, table_ref),
        (state_hbm, state_ref.at[:, pl.ds(0, levels), :]),
    )
    copies = [pltpu.make_async_copy(src, dst, sems.at[i]) for i, (src, dst) in enumerate(pairs)]
    for copy in copies:
        copy.start()
    copies[0].wait()
    inv_ref[...] = slot_owner(slot_ref)
    copies[1].wait()
    copies[2].wait()
    halo_weights(inv_ref, vw_ref, table_ref, out_refs, (0, 1))
    copies[3].wait()
    for m in range(members):
        state_ref[m, levels:, :] = jnp.zeros((state_ref.shape[1] - levels, cells), BF16)


def ask_high_kernel(inv_ref, vw_ref, table_ref, own_ref, *out_refs):
    halo_weights(inv_ref, vw_ref, table_ref, out_refs, (2, 3))
    for tile in range(own_ref.shape[1] // TILE):
        own_ref[:, tile * TILE : (tile + 1) * TILE] = slot_weights(inv_ref, vw_ref, tile)


def halo_weights(inv_ref, vw_ref, table_ref, out_refs, numbers):
    obs = vw_ref.shape[1]
    for out, number in zip(out_refs, numbers):
        count = out.shape[1] // TILE
        for part in range(count):
            tile = obs // TILE + number * count + part
            out[:, part * TILE : (part + 1) * TILE] = slot_weights(inv_ref, vw_ref, tile, table_ref)


def answer_tile(cell_of, w, turned_ref, cells_dim):
    S, rest = row_stride(cells_dim), member_row(cells_dim, 8)
    half = TILE // 2
    lane = lax.broadcasted_iota(jnp.int32, (8, TILE), 1) & (half - 1)
    wide = lax.broadcasted_iota(jnp.int32, (128, TILE), 1)
    zero = jnp.zeros_like(w)
    rhs = jnp.concatenate([jnp.where(wide < half, w, zero), jnp.where(wide < half, zero, w)], axis=0)
    first, second = [], []
    for h in range(2):
        a_rows, b_rows = [], []
        for q in range(half // 4):
            for j in range(4):
                c = cell_of(h * half + 4 * q + j)
                a_rows.append(turned_ref[pl.ds(c, 8, stride=S), :])
                b_rows.append(turned_ref[pl.ds(c + rest, 2, stride=S), :])
        first.append(jnp.concatenate(a_rows, axis=0).astype(BF16))
        second.append(jnp.concatenate(b_rows, axis=0).astype(BF16))
    lhs_a = jnp.concatenate(first, axis=1)
    lhs_b = jnp.concatenate(second, axis=1)
    d_a = jnp.dot(lhs_a, rhs, preferred_element_type=F32)
    d_b = jnp.dot(lhs_b, rhs, preferred_element_type=F32)
    out_a = jnp.zeros((8, TILE), F32)
    for r in range(half):
        out_a = jnp.where(lane == r, d_a[8 * r : 8 * r + 8, :], out_a)
    out_b = jnp.zeros((8, TILE), F32)
    near = lane - (lax.broadcasted_iota(jnp.int32, (8, TILE), 0) >> 1)
    for q in range(half // 4):
        out_b = jnp.where(near == 4 * q, d_b[8 * q : 8 * q + 8, :], out_b)
    return jnp.concatenate([out_a, out_b], axis=0)


def own_kernel(state_ref, table_hbm, w_ref, turned_ref, eq_ref, cell_ref, cell_sem):
    members, levels, cells = state_ref.shape
    copy = pltpu.make_async_copy(table_hbm.at[:, pl.ds(0, eq_ref.shape[1])], cell_ref, cell_sem)
    copy.start()
    r = lax.broadcasted_iota(jnp.int32, (TILE, TILE), 0)
    eye = jnp.where(r == lax.broadcasted_iota(jnp.int32, (TILE, TILE), 1), 1.0, 0.0).astype(BF16)
    for m in range(0, members, 2):
        for part in range(cells // TILE):
            at = slice(part * TILE, (part + 1) * TILE)
            block = jnp.concatenate([state_ref[m, :, at], state_ref[m + 1, :, at]], axis=0)
            flat = lax.dot_general(eye, block, NT, preferred_element_type=F32)
            for i in range(2):
                low = member_row(cells, m + i) + part * TILE
                turned_ref[low : low + TILE, :] = flat[:, i * 128 : (i + 1) * 128]
    copy.wait()
    for tile in range(eq_ref.shape[1] // TILE):
        at = slice(tile * TILE, (tile + 1) * TILE)
        eq_ref[:, at] = answer_tile(lambda i: cell_ref[0, tile * TILE + i], w_ref[:, at], turned_ref, cells)


def answer_kernel(levels, cells, turned_ref, *refs):
    count = len(refs) // 4
    w_refs, eq_refs = refs[:count], refs[count : 2 * count]
    words, scalars, sems = refs[2 * count : 3 * count], refs[3 * count : 4 * count], refs[-1]
    copies = []
    for i in range(count):
        tail = w_refs[i][112:128, :].astype(F32)
        row = levels - 112
        words[i][...] = (8.0 * tail[row : row + 1, :] + tail[row + 1 : row + 2, :]).astype(jnp.int32)
        copies.append(pltpu.make_async_copy(words[i], scalars[i], sems.at[i]))
        copies[-1].start()
    keep = lax.broadcasted_iota(jnp.int32, (128, TILE), 0) < levels
    for copy in copies:
        copy.wait()
    for i in range(count):
        for tile in range(eq_refs[i].shape[1] // TILE):
            at = slice(tile * TILE, (tile + 1) * TILE)
            w = w_refs[i][:, at]
            w = jnp.where(keep, w, jnp.zeros_like(w))
            eq_refs[i][:, at] = answer_tile(lambda j: scalars[i][0, tile * TILE + j], w, turned_ref, cells)


def combine_kernel(firsts, slot_ref, hw_ref, *refs):
    *eq_refs, out_ref = refs
    before = eq_refs.pop(0) if len(eq_refs) > len(firsts) else None
    neigh, obs = slot_ref.shape
    sub = lax.broadcasted_iota(jnp.int32, (8, 128), 0)
    tops, pairs = {}, {}
    for first, ref in zip(firsts, eq_refs):
        for part in range(ref.shape[1] // 128):
            tops[first + part] = ref[0:8, part * 128 : (part + 1) * 128]
            x = ref[8:16, part * 128 : (part + 1) * 128]
            x = x + pltpu.roll(x, 4, 0)
            pairs[first + part] = x + pltpu.roll(x, 2, 0)
    quads = {}
    for q in sorted({i // 4 for i in pairs}):
        x = jnp.zeros((8, 128), F32)
        for j in range(4):
            if 4 * q + j in pairs:
                x = jnp.where(sub >> 1 == j, pairs[4 * q + j], x)
        quads[q] = x
    last = None
    for block in range(obs // 128):
        at = slice(block * 128, (block + 1) * 128)
        a_sum = jnp.zeros((8, 128), F32)
        b_sum = jnp.zeros((8, 128), F32)
        for k in range(neigh):
            s = jnp.broadcast_to(slot_ref[k : k + 1, at], (8, 128))
            low, top = s & 127, s >> 7
            a = jnp.zeros((8, 128), F32)
            for i, x in tops.items():
                a = jnp.where(top == i, jnp.take_along_axis(x, low, axis=1, mode="promise_in_bounds"), a)
            b = jnp.zeros((8, 128), F32)
            top4 = top >> 2
            for i, x in quads.items():
                b = jnp.where(top4 == i, jnp.take_along_axis(x, low, axis=1, mode="promise_in_bounds"), b)
            b = jnp.where((top & 3) == (sub >> 1), b, 0.0)
            h = hw_ref[k : k + 1, at]
            a_sum += a * h
            b_sum += b * h
        b_sum = b_sum + pltpu.roll(b_sum, 4, 0)
        b_sum = b_sum + pltpu.roll(b_sum, 2, 0)
        if before is not None:
            a_sum += before[:, at]
        out_ref[:, at] = a_sum
        last = b_sum if block % 4 == 0 else jnp.where(sub >> 1 >= block % 4, b_sum, last)
        if block % 4 == 3:
            low = obs + block // 4 * 128
            if before is not None:
                last += before[:, low : low + 128]
            out_ref[:, low : low + 128] = last


def unpacked(ref, obs):
    sub = lax.broadcasted_iota(jnp.int32, (8, 128), 0)
    rest = []
    for block in range(obs // 128):
        low = obs + block // 4 * 128
        x = ref[:, low : low + 128]
        if block % 4:
            x = pltpu.roll(x, 8 - 2 * (block % 4), 0)
        rest.append(jnp.where(sub < 2, x, 0.0))
    return jnp.concatenate([ref[:, :obs], jnp.concatenate(rest, axis=1)], axis=0)


def split(x):
    top = x.astype(BF16)
    return top, (x - top.astype(F32)).astype(BF16)


def cov_kernel(members, own_ref, r1_ref, r2_ref, r3_ref, value_ref, error_ref, region_ref, mid_ref, prev_ref, next_ref):
    mem_dev = members // 4
    obs = region_ref.shape[1]
    blocks = [unpacked(ref, obs) for ref in (own_ref, r1_ref, r2_ref, r3_ref)]
    total = blocks[0] + blocks[1] + blocks[2] + blocks[3]
    mean = jnp.sum(total, axis=0, keepdims=True) * (1.0 / members)
    err = error_ref[...]
    inverse = 1.0 / (err * err)
    innov = (value_ref[...] - mean) * inverse
    row = lax.broadcasted_iota(jnp.int32, (16, obs), 0)
    spread = [jnp.where(row < mem_dev, x - mean, 0.0) for x in blocks]
    right = [x * inverse for x in spread]
    right[0] = jnp.where(row == mem_dev, innov, right[0])
    r_top, r_low = split(jnp.concatenate(right, axis=0))
    regions = lax.axis_size("cell") * REG_DEV
    rel = region_ref[...] - (lax.axis_index("cell") - 1) * REG_DEV
    rel = jnp.where(rel < 0, rel + regions, rel)
    rel = jnp.where(rel >= regions, rel - regions, rel)
    region = lax.broadcasted_iota(jnp.int32, (REG_DEV, obs), 0)
    own = spread[0]
    own_low = own - own.astype(BF16).astype(F32)
    for g, out_ref in ((0, prev_ref), (2, next_ref), (1, mid_ref)):
        mask = rel == region + g * REG_DEV
        l_top = jnp.concatenate([jnp.where(mask, own[m : m + 1, :], 0.0) for m in range(mem_dev)], axis=0).astype(BF16)
        l_low = jnp.concatenate([jnp.where(mask, own_low[m : m + 1, :], 0.0) for m in range(mem_dev)], axis=0).astype(BF16)
        d = lax.dot_general(l_top, r_top, NT, preferred_element_type=F32)
        d += lax.dot_general(l_top, r_low, NT, preferred_element_type=F32)
        d += lax.dot_general(l_low, r_top, NT, preferred_element_type=F32)
        out_ref[...] = d


def final_kernel(mid_ref, a_ref, b_ref, cov_ref, proj_ref):
    mem_dev, regions, members = cov_ref.shape
    d = mid_ref[...] + a_ref[...] + b_ref[...]
    width = d.shape[1]
    i = lax.broadcasted_iota(jnp.int32, (width, members), 0)
    j = lax.broadcasted_iota(jnp.int32, (width, members), 1)
    block = (lax.axis_index("mem") + 4 - (i >> 4)) & 3
    place = jnp.where(((i & 15) < mem_dev) & (block * mem_dev + (i & 15) == j), 1.0, 0.0)
    cov = jnp.dot(d, place, precision=lax.Precision.HIGHEST, preferred_element_type=F32)
    lane = lax.broadcasted_iota(jnp.int32, (regions, mem_dev), 1)
    proj = jnp.zeros((regions, mem_dev), F32)
    for m in range(mem_dev):
        cov_ref[m] = cov[m * regions : (m + 1) * regions, :]
        proj = jnp.where(lane == m, d[m * regions : (m + 1) * regions, mem_dev : mem_dev + 1], proj)
    proj_ref[...] = proj


def on_device(state, vertical_weight, horizontal_weight, obs_slot, request_cell, obs_value, obs_error, obs_region):
    cells, mem_dev, levels = state.shape
    members = mem_dev * lax.axis_size("mem")
    obs, neigh = obs_slot.shape
    halo = 3 * obs // 4
    state_t = jnp.transpose(state, (1, 2, 0))
    vw_t, hw_t, slot_t = vertical_weight.T, horizontal_weight.T, obs_slot.T
    far = lambda x: pltpu.with_memory_space_constraint(x, pltpu.HBM)
    params = pltpu.CompilerParams(vmem_limit_bytes=16 * 1024 * 1024)

    w_shape = jax.ShapeDtypeStruct((128, halo), BF16)
    inv, vw_near, table, state_near, ask_m2, ask_m1 = pl.pallas_call(
        ask_low_kernel,
        out_shape=[
            pltpu.VMEM((neigh * obs // 128, 128), jnp.int32),
            pltpu.VMEM((levels, obs), BF16),
            pltpu.VMEM((1, neigh * obs), jnp.int32),
            pltpu.VMEM((mem_dev, 128, cells), BF16),
            w_shape,
            w_shape,
        ],
        in_specs=[ANY] * 4,
        out_specs=[VMEM] * 6,
        scratch_shapes=[pltpu.VMEM((neigh, obs), jnp.int32), pltpu.SemaphoreType.DMA((4,))],
        compiler_params=params,
        cost_estimate=pl.CostEstimate(flops=2_000_000_000, bytes_accessed=6_000_000, transcendentals=0),
        name="ask_low",
    )(far(slot_t), far(request_cell), far(vw_t), far(state_t))
    w_m2, w_m1 = passed_along(ask_m2, "cell", -2), passed_along(ask_m1, "cell", -1)
    w_own, ask_p1, ask_p2 = pl.pallas_call(
        ask_high_kernel,
        out_shape=[pltpu.VMEM((128, obs), BF16), w_shape, w_shape],
        in_specs=[VMEM] * 3,
        out_specs=[VMEM] * 3,
        compiler_params=params,
        cost_estimate=pl.CostEstimate(flops=2_000_000_000, bytes_accessed=1_000_000, transcendentals=0),
        name="ask_high",
    )(inv, vw_near, table)
    w_p1, w_p2 = passed_along(ask_p1, "cell", 1), passed_along(ask_p2, "cell", 2)
    turned, eq_own = pl.pallas_call(
        own_kernel,
        out_shape=[
            pltpu.VMEM((mem_dev * row_stride(cells), 128), F32),
            pltpu.VMEM((16, obs), F32),
        ],
        in_specs=[VMEM, ANY, VMEM],
        out_specs=[VMEM] * 2,
        scratch_shapes=[pltpu.SMEM((1, obs), jnp.int32), pltpu.SemaphoreType.DMA],
        compiler_params=params,
        cost_estimate=pl.CostEstimate(flops=8_000_000_000, bytes_accessed=10_000_000, transcendentals=0),
        name="own",
    )(state_near, far(request_cell), w_own)
    turned = pltpu.with_memory_space_constraint(turned, pltpu.VMEM)
    answer = pl.pallas_call(
        lambda *refs: answer_kernel(levels, cells, *refs),
        out_shape=[jax.ShapeDtypeStruct((16, halo), F32)] * 2,
        in_specs=[VMEM] * 3,
        out_specs=[VMEM] * 2,
        scratch_shapes=[pltpu.VMEM((1, halo), jnp.int32)] * 2
        + [pltpu.SMEM((1, halo), jnp.int32)] * 2
        + [pltpu.SemaphoreType.DMA((2,))],
        compiler_params=params,
        cost_estimate=pl.CostEstimate(flops=4_000_000_000, bytes_accessed=1_000_000, transcendentals=0),
        name="answer",
    )
    eq_m2, eq_m1 = answer(turned, w_m2, w_m1)
    eq_m2, eq_m1 = passed_along(eq_m2, "cell", 2), passed_along(eq_m1, "cell", 1)
    eq_p1, eq_p2 = answer(turned, w_p1, w_p2)
    eq_p1, eq_p2 = passed_along(eq_p1, "cell", -1), passed_along(eq_p2, "cell", -2)

    def combine(tables, *before):
        firsts = [obs // 128 + n * halo // 128 if n >= 0 else 0 for n, _ in tables]
        return pl.pallas_call(
            lambda *refs: combine_kernel(firsts, *refs),
            out_shape=jax.ShapeDtypeStruct((8, obs + obs // 4), F32),
            in_specs=[VMEM] * (2 + len(before) + len(tables)),
            out_specs=VMEM,
            compiler_params=params,
            cost_estimate=pl.CostEstimate(flops=1_000_000_000, bytes_accessed=1_000_000, transcendentals=0),
            name="combine",
        )(slot_t, hw_t, *before, *(x for _, x in tables))

    own = combine([(-1, eq_own), (0, eq_m2), (1, eq_m1)])
    own = combine([(2, eq_p1), (3, eq_p2)], own)
    others = [passed_along(own, "mem", by) for by in (1, 2, 3)]
    wide = 4 * 16
    mid, to_prev, to_next = pl.pallas_call(
        lambda *refs: cov_kernel(members, *refs),
        out_shape=[jax.ShapeDtypeStruct((mem_dev * REG_DEV, wide), F32)] * 3,
        in_specs=[VMEM] * 7,
        out_specs=[VMEM] * 3,
        compiler_params=params,
        name="cov",
    )(own, *others, obs_value.reshape(1, obs), obs_error.reshape(1, obs), obs_region.reshape(1, obs))
    from_prev = passed_along(to_next, "cell", 1)
    from_next = passed_along(to_prev, "cell", -1)
    cov, proj = pl.pallas_call(
        final_kernel,
        out_shape=[
            jax.ShapeDtypeStruct((mem_dev, REG_DEV, members), F32),
            jax.ShapeDtypeStruct((REG_DEV, mem_dev), F32),
        ],
        in_specs=[VMEM] * 3,
        out_specs=[VMEM] * 2,
        compiler_params=params,
        name="final",
    )(mid, from_prev, from_next)
    return (jnp.transpose(cov, (1, 0, 2)), proj)


def solution(mesh):
    in_specs = (
        P("cell", "mem", None),
        P("cell", None),
        P("cell", None),
        P("cell", None),
        P("cell", None),
        P("cell"),
        P("cell"),
        P("cell"),
    )
    out_specs = (P("cell", "mem", None), P("cell", "mem"))
    return jax.shard_map(
        on_device, mesh=mesh, in_specs=in_specs, out_specs=out_specs, check_vma=False
    )
```

```python
import jax
import jax.numpy as jnp
from jax import lax
from jax.experimental import pallas as pl
from jax.experimental.pallas import tpu as pltpu
from jax.sharding import PartitionSpec as P

REG_DEV = 8
TILE = 256
F32 = jnp.float32
BF16 = jnp.bfloat16
NT = (((1,), (1,)), ((), ()))
VMEM = pl.BlockSpec(memory_space=pltpu.VMEM)
ANY = pl.BlockSpec(memory_space=pltpu.HBM)
SMEM = pl.BlockSpec(memory_space=pltpu.SMEM)


def passed_along(x, axis, by):
    devices = lax.axis_size(axis)
    return lax.ppermute(x, axis, [(i, (i + by) % devices) for i in range(devices)])


def swapped(x, axis, mask):
    return lax.ppermute(x, axis, [(i, i ^ mask) for i in range(lax.axis_size(axis))])


def row_stride(cells):
    return cells + 4


def member_row(cells, m):
    return m * row_stride(cells) + (m >= 8)


def slot_owner(slot_ref):
    neigh, obs = slot_ref.shape
    tops = neigh * obs // 128
    o = lax.broadcasted_iota(jnp.int32, (1, obs), 1)
    upper, lower = (o >> 5).astype(F32), (o & 31).astype(F32)
    row_top = lax.broadcasted_iota(jnp.int32, (tops, obs), 0)
    row_low = lax.broadcasted_iota(jnp.int32, (128, obs), 0)
    total = jnp.zeros((2 * tops, 128), F32)
    for k in range(neigh):
        s = slot_ref[k : k + 1, :]
        hit = row_top == (s >> 7)
        lhs = jnp.concatenate(
            [jnp.where(hit, upper, 0.0), jnp.where(hit, lower, 0.0)], axis=0
        ).astype(BF16)
        rhs = jnp.where(row_low == (s & 127), 1.0, 0.0).astype(BF16)
        total += lax.dot_general(lhs, rhs, NT, preferred_element_type=F32)
    return (32.0 * total[:tops] + total[tops:]).astype(jnp.int32)


def slot_weights(inv_ref, vw_ref, tile, table_ref=None):
    levels, obs = vw_ref.shape
    key = jnp.concatenate([inv_ref[2 * tile : 2 * tile + 1, :], inv_ref[2 * tile + 1 : 2 * tile + 2, :]], axis=1)
    ids = lax.broadcasted_iota(jnp.int32, (obs, TILE), 0)
    pick = jnp.where(ids == key, 1.0, 0.0).astype(BF16)
    w = jnp.dot(vw_ref[...], pick, preferred_element_type=F32)
    extra = jnp.zeros((128 - levels, TILE), F32)
    if table_ref is not None:
        cells = table_ref[0:1, tile * TILE : (tile + 1) * TILE]
        sub = lax.broadcasted_iota(jnp.int32, (128 - levels, TILE), 0)
        extra = jnp.where(sub == 0, (cells >> 3).astype(F32), jnp.where(sub == 1, (cells & 7).astype(F32), extra))
    return jnp.concatenate([w, extra], axis=0).astype(BF16)


def ask_low_kernel(slot_hbm, table_hbm, vw_hbm, inv_ref, vw_ref, table_ref, *refs):
    *out_refs, slot_ref, sems = refs
    pairs = ((slot_hbm, slot_ref), (vw_hbm, vw_ref), (table_hbm, table_ref))
    copies = [pltpu.make_async_copy(src, dst, sems.at[i]) for i, (src, dst) in enumerate(pairs)]
    for copy in copies:
        copy.start()
    copies[0].wait()
    inv_ref[...] = slot_owner(slot_ref)
    copies[1].wait()
    copies[2].wait()
    halo_weights(inv_ref, vw_ref, table_ref, out_refs, (0, 1))


def ask_high_kernel(inv_ref, vw_ref, table_ref, own_ref, *out_refs):
    halo_weights(inv_ref, vw_ref, table_ref, out_refs, (2, 3))
    for tile in range(own_ref.shape[1] // TILE):
        own_ref[:, tile * TILE : (tile + 1) * TILE] = slot_weights(inv_ref, vw_ref, tile)


def halo_weights(inv_ref, vw_ref, table_ref, out_refs, numbers):
    obs = vw_ref.shape[1]
    for out, number in zip(out_refs, numbers):
        count = out.shape[1] // TILE
        for part in range(count):
            tile = obs // TILE + number * count + part
            out[:, part * TILE : (part + 1) * TILE] = slot_weights(inv_ref, vw_ref, tile, table_ref)


def answer_tile(cell_of, w, turned_ref, cells_dim):
    S, rest = row_stride(cells_dim), member_row(cells_dim, 8)
    half = TILE // 2
    lane = lax.broadcasted_iota(jnp.int32, (8, 128), 1)
    near = lane - (lax.broadcasted_iota(jnp.int32, (8, 128), 0) >> 1)
    wide = lax.broadcasted_iota(jnp.int32, (128, TILE), 1)
    zero = jnp.zeros_like(w)
    rhs = jnp.concatenate([jnp.where(wide < half, w, zero), jnp.where(wide < half, zero, w)], axis=0)
    parts = []
    for o in range(half // 8):
        sides = []
        for h in range(2):
            a_rows, b_rows = [], []
            for j in range(8):
                c = cell_of(h * half + 8 * o + j)
                a_rows.append(turned_ref[pl.ds(c, 8, stride=S), :])
                b_rows.append(turned_ref[pl.ds(c + rest, 2, stride=S), :])
            sides.append(jnp.concatenate(a_rows + b_rows, axis=0).astype(BF16))
        parts.append(jnp.concatenate(sides, axis=1))
    d = jnp.dot(jnp.concatenate(parts, axis=0), rhs, preferred_element_type=F32)
    out_a = [jnp.zeros((8, 128), F32)] * 2
    out_b = [jnp.zeros((8, 128), F32)] * 2
    for o in range(half // 8):
        for j in range(8):
            low = 80 * o + 8 * j
            hit = lane == 8 * o + j
            for h in range(2):
                out_a[h] = jnp.where(hit, d[low : low + 8, h * half : (h + 1) * half], out_a[h])
        for i in range(2):
            low = 80 * o + 64 + 8 * i
            hit = near == 8 * o + 4 * i
            for h in range(2):
                out_b[h] = jnp.where(hit, d[low : low + 8, h * half : (h + 1) * half], out_b[h])
    return jnp.concatenate([jnp.concatenate(out_a, axis=1), jnp.concatenate(out_b, axis=1)], axis=0)


def own_kernel(state_hbm, table_hbm, w_ref, turned_ref, eq_ref, state_ref, cell_ref, cell_sem, sems):
    members, levels, cells = state_hbm.shape
    for m in range(members):
        state_ref[m, levels:, :] = jnp.zeros((state_ref.shape[1] - levels, cells), BF16)
    copies = [
        pltpu.make_async_copy(
            state_hbm.at[pl.ds(m, 2)], state_ref.at[pl.ds(m, 2), pl.ds(0, levels), :], sems.at[m // 2]
        )
        for m in range(0, members, 2)
    ]
    for each in copies:
        each.start()
    copy = pltpu.make_async_copy(table_hbm.at[:, pl.ds(0, eq_ref.shape[1])], cell_ref, cell_sem)
    copy.start()
    r = lax.broadcasted_iota(jnp.int32, (TILE, TILE), 0)
    eye = jnp.where(r == lax.broadcasted_iota(jnp.int32, (TILE, TILE), 1), 1.0, 0.0).astype(BF16)
    for m in range(0, members, 2):
        copies[m // 2].wait()
        for part in range(cells // TILE):
            at = slice(part * TILE, (part + 1) * TILE)
            block = jnp.concatenate([state_ref[m, :, at], state_ref[m + 1, :, at]], axis=0)
            flat = lax.dot_general(eye, block, NT, preferred_element_type=F32)
            for i in range(2):
                low = member_row(cells, m + i) + part * TILE
                turned_ref[low : low + TILE, :] = flat[:, i * 128 : (i + 1) * 128]
    copy.wait()
    for tile in range(eq_ref.shape[1] // TILE):
        at = slice(tile * TILE, (tile + 1) * TILE)
        eq_ref[:, at] = answer_tile(lambda i: cell_ref[0, tile * TILE + i], w_ref[:, at], turned_ref, cells)


def answer_kernel(levels, cells, turned_ref, *refs):
    count = len(refs) // 4
    w_refs, eq_refs = refs[:count], refs[count : 2 * count]
    words, scalars, sems = refs[2 * count : 3 * count], refs[3 * count : 4 * count], refs[-1]
    copies = []
    for i in range(count):
        tail = w_refs[i][112:128, :].astype(F32)
        row = levels - 112
        words[i][...] = (8.0 * tail[row : row + 1, :] + tail[row + 1 : row + 2, :]).astype(jnp.int32)
        copies.append(pltpu.make_async_copy(words[i], scalars[i], sems.at[i]))
        copies[-1].start()
    keep = lax.broadcasted_iota(jnp.int32, (128, TILE), 0) < levels
    for copy in copies:
        copy.wait()
    for i in range(count):
        for tile in range(eq_refs[i].shape[1] // TILE):
            at = slice(tile * TILE, (tile + 1) * TILE)
            w = w_refs[i][:, at]
            w = jnp.where(keep, w, jnp.zeros_like(w))
            eq_refs[i][:, at] = answer_tile(lambda j: scalars[i][0, tile * TILE + j], w, turned_ref, cells)


def combine_kernel(firsts, slot_ref, hw_ref, *refs):
    *eq_refs, out_ref = refs
    before = eq_refs.pop(0) if len(eq_refs) > len(firsts) else None
    neigh, obs = slot_ref.shape
    sub = lax.broadcasted_iota(jnp.int32, (8, 128), 0)
    tops, pairs = {}, {}
    for first, ref in zip(firsts, eq_refs):
        for part in range(ref.shape[1] // 128):
            tops[first + part] = ref[0:8, part * 128 : (part + 1) * 128]
            x = ref[8:16, part * 128 : (part + 1) * 128]
            x = x + pltpu.roll(x, 4, 0)
            pairs[first + part] = x + pltpu.roll(x, 2, 0)
    quads = {}
    for q in sorted({i // 4 for i in pairs}):
        x = jnp.zeros((8, 128), F32)
        for j in range(4):
            if 4 * q + j in pairs:
                x = jnp.where(sub >> 1 == j, pairs[4 * q + j], x)
        quads[q] = x
    last = None
    for block in range(obs // 128):
        at = slice(block * 128, (block + 1) * 128)
        a_sum = jnp.zeros((8, 128), F32)
        b_sum = jnp.zeros((8, 128), F32)
        for k in range(neigh):
            s = jnp.broadcast_to(slot_ref[k : k + 1, at], (8, 128))
            low, top = s & 127, s >> 7
            a = jnp.zeros((8, 128), F32)
            for i, x in tops.items():
                a = jnp.where(top == i, jnp.take_along_axis(x, low, axis=1, mode="promise_in_bounds"), a)
            b = jnp.zeros((8, 128), F32)
            top4 = top >> 2
            for i, x in quads.items():
                b = jnp.where(top4 == i, jnp.take_along_axis(x, low, axis=1, mode="promise_in_bounds"), b)
            b = jnp.where((top & 3) == (sub >> 1), b, 0.0)
            h = hw_ref[k : k + 1, at]
            a_sum += a * h
            b_sum += b * h
        b_sum = b_sum + pltpu.roll(b_sum, 4, 0)
        b_sum = b_sum + pltpu.roll(b_sum, 2, 0)
        if before is not None:
            a_sum += before[:, at]
        out_ref[:, at] = a_sum
        last = b_sum if block % 4 == 0 else jnp.where(sub >> 1 >= block % 4, b_sum, last)
        if block % 4 == 3:
            low = obs + block // 4 * 128
            if before is not None:
                last += before[:, low : low + 128]
            out_ref[:, low : low + 128] = last


def unpacked(ref, obs):
    sub = lax.broadcasted_iota(jnp.int32, (8, 128), 0)
    rest = []
    for block in range(obs // 128):
        low = obs + block // 4 * 128
        x = ref[:, low : low + 128]
        if block % 4:
            x = pltpu.roll(x, 8 - 2 * (block % 4), 0)
        rest.append(jnp.where(sub < 2, x, 0.0))
    return jnp.concatenate([ref[:, :obs], jnp.concatenate(rest, axis=1)], axis=0)


def split(x):
    top = x.astype(BF16)
    return top, (x - top.astype(F32)).astype(BF16)


def cov_kernel(members, own_ref, r1_ref, r2_ref, r3_ref, value_ref, error_ref, region_ref, mid_ref, prev_ref, next_ref):
    mem_dev = members // 4
    obs = region_ref.shape[1]
    blocks = [unpacked(ref, obs) for ref in (own_ref, r1_ref, r2_ref, r3_ref)]
    total = blocks[0] + blocks[1] + blocks[2] + blocks[3]
    mean = jnp.sum(total, axis=0, keepdims=True) * (1.0 / members)
    err = error_ref[...]
    inverse = 1.0 / (err * err)
    innov = (value_ref[...] - mean) * inverse
    row = lax.broadcasted_iota(jnp.int32, (16, obs), 0)
    spread = [jnp.where(row < mem_dev, x - mean, 0.0) for x in blocks]
    right = [x * inverse for x in spread]
    right[0] = jnp.where(row == mem_dev, innov, right[0])
    r_top, r_low = split(jnp.concatenate(right, axis=0))
    regions = lax.axis_size("cell") * REG_DEV
    rel = region_ref[...] - (lax.axis_index("cell") - 1) * REG_DEV
    rel = jnp.where(rel < 0, rel + regions, rel)
    rel = jnp.where(rel >= regions, rel - regions, rel)
    region = lax.broadcasted_iota(jnp.int32, (REG_DEV, obs), 0)
    own = spread[0]
    own_low = own - own.astype(BF16).astype(F32)
    for g, out_ref in ((0, prev_ref), (2, next_ref), (1, mid_ref)):
        mask = rel == region + g * REG_DEV
        l_top = jnp.concatenate([jnp.where(mask, own[m : m + 1, :], 0.0) for m in range(mem_dev)], axis=0).astype(BF16)
        l_low = jnp.concatenate([jnp.where(mask, own_low[m : m + 1, :], 0.0) for m in range(mem_dev)], axis=0).astype(BF16)
        d = lax.dot_general(l_top, r_top, NT, preferred_element_type=F32)
        d += lax.dot_general(l_top, r_low, NT, preferred_element_type=F32)
        d += lax.dot_general(l_low, r_top, NT, preferred_element_type=F32)
        out_ref[...] = d


def final_kernel(mid_ref, a_ref, b_ref, cov_ref, proj_ref):
    mem_dev, regions, members = cov_ref.shape
    d = mid_ref[...] + a_ref[...] + b_ref[...]
    width = d.shape[1]
    i = lax.broadcasted_iota(jnp.int32, (width, members), 0)
    j = lax.broadcasted_iota(jnp.int32, (width, members), 1)
    block = lax.axis_index("mem") ^ (i >> 4)
    place = jnp.where(((i & 15) < mem_dev) & (block * mem_dev + (i & 15) == j), 1.0, 0.0)
    cov = jnp.dot(d, place, precision=lax.Precision.HIGHEST, preferred_element_type=F32)
    lane = lax.broadcasted_iota(jnp.int32, (regions, mem_dev), 1)
    proj = jnp.zeros((regions, mem_dev), F32)
    for m in range(mem_dev):
        cov_ref[m] = cov[m * regions : (m + 1) * regions, :]
        proj = jnp.where(lane == m, d[m * regions : (m + 1) * regions, mem_dev : mem_dev + 1], proj)
    proj_ref[...] = proj


def on_device(state, vertical_weight, horizontal_weight, obs_slot, request_cell, obs_value, obs_error, obs_region):
    cells, mem_dev, levels = state.shape
    members = mem_dev * lax.axis_size("mem")
    obs, neigh = obs_slot.shape
    halo = 3 * obs // 4
    state_t = jnp.transpose(state, (1, 2, 0))
    vw_t, hw_t, slot_t = vertical_weight.T, horizontal_weight.T, obs_slot.T
    far = lambda x: pltpu.with_memory_space_constraint(x, pltpu.HBM)
    params = pltpu.CompilerParams(vmem_limit_bytes=16 * 1024 * 1024)

    w_shape = jax.ShapeDtypeStruct((128, halo), BF16)
    inv, vw_near, table, ask_m2, ask_m1 = pl.pallas_call(
        ask_low_kernel,
        out_shape=[
            pltpu.VMEM((neigh * obs // 128, 128), jnp.int32),
            pltpu.VMEM((levels, obs), BF16),
            pltpu.VMEM((1, neigh * obs), jnp.int32),
            w_shape,
            w_shape,
        ],
        in_specs=[ANY] * 3,
        out_specs=[VMEM] * 5,
        scratch_shapes=[pltpu.VMEM((neigh, obs), jnp.int32), pltpu.SemaphoreType.DMA((3,))],
        compiler_params=params,
        cost_estimate=pl.CostEstimate(flops=2_000_000_000, bytes_accessed=6_000_000, transcendentals=0),
        name="ask_low",
    )(far(slot_t), far(request_cell), far(vw_t))
    w_m2, w_m1 = passed_along(ask_m2, "cell", -2), passed_along(ask_m1, "cell", -1)
    w_own, ask_p1, ask_p2 = pl.pallas_call(
        ask_high_kernel,
        out_shape=[pltpu.VMEM((128, obs), BF16), w_shape, w_shape],
        in_specs=[VMEM] * 3,
        out_specs=[VMEM] * 3,
        compiler_params=params,
        cost_estimate=pl.CostEstimate(flops=2_000_000_000, bytes_accessed=1_000_000, transcendentals=0),
        name="ask_high",
    )(inv, vw_near, table)
    w_p1, w_p2 = passed_along(ask_p1, "cell", 1), passed_along(ask_p2, "cell", 2)
    turned, eq_own = pl.pallas_call(
        own_kernel,
        out_shape=[
            pltpu.VMEM((mem_dev * row_stride(cells), 128), F32),
            pltpu.VMEM((16, obs), F32),
        ],
        in_specs=[ANY, ANY, VMEM],
        out_specs=[VMEM] * 2,
        scratch_shapes=[
            pltpu.VMEM((mem_dev, 128, cells), BF16),
            pltpu.SMEM((1, obs), jnp.int32),
            pltpu.SemaphoreType.DMA,
            pltpu.SemaphoreType.DMA((mem_dev // 2,)),
        ],
        compiler_params=params,
        cost_estimate=pl.CostEstimate(flops=8_000_000_000, bytes_accessed=10_000_000, transcendentals=0),
        name="own",
    )(far(state_t), far(request_cell), w_own)
    turned = pltpu.with_memory_space_constraint(turned, pltpu.VMEM)
    answer = pl.pallas_call(
        lambda *refs: answer_kernel(levels, cells, *refs),
        out_shape=[jax.ShapeDtypeStruct((16, halo), F32)] * 2,
        in_specs=[VMEM] * 3,
        out_specs=[VMEM] * 2,
        scratch_shapes=[pltpu.VMEM((1, halo), jnp.int32)] * 2
        + [pltpu.SMEM((1, halo), jnp.int32)] * 2
        + [pltpu.SemaphoreType.DMA((2,))],
        compiler_params=params,
        cost_estimate=pl.CostEstimate(flops=4_000_000_000, bytes_accessed=1_000_000, transcendentals=0),
        name="answer",
    )
    eq_m2, eq_m1 = answer(turned, w_m2, w_m1)
    eq_m2, eq_m1 = passed_along(eq_m2, "cell", 2), passed_along(eq_m1, "cell", 1)
    eq_p1, eq_p2 = answer(turned, w_p1, w_p2)
    eq_p1, eq_p2 = passed_along(eq_p1, "cell", -1), passed_along(eq_p2, "cell", -2)

    def combine(tables, *before):
        firsts = [obs // 128 + n * halo // 128 if n >= 0 else 0 for n, _ in tables]
        return pl.pallas_call(
            lambda *refs: combine_kernel(firsts, *refs),
            out_shape=jax.ShapeDtypeStruct((8, obs + obs // 4), F32),
            in_specs=[VMEM] * (2 + len(before) + len(tables)),
            out_specs=VMEM,
            compiler_params=params,
            cost_estimate=pl.CostEstimate(flops=1_000_000_000, bytes_accessed=1_000_000, transcendentals=0),
            name="combine",
        )(slot_t, hw_t, *before, *(x for _, x in tables))

    own = combine([(-1, eq_own), (0, eq_m2), (1, eq_m1)])
    own = combine([(2, eq_p1), (3, eq_p2)], own)
    others = [swapped(own, "mem", mask) for mask in (1, 2, 3)]
    wide = 4 * 16
    mid, to_prev, to_next = pl.pallas_call(
        lambda *refs: cov_kernel(members, *refs),
        out_shape=[jax.ShapeDtypeStruct((mem_dev * REG_DEV, wide), F32)] * 3,
        in_specs=[VMEM] * 7,
        out_specs=[VMEM] * 3,
        compiler_params=params,
        name="cov",
    )(own, *others, obs_value.reshape(1, obs), obs_error.reshape(1, obs), obs_region.reshape(1, obs))
    from_prev = passed_along(to_next, "cell", 1)
    from_next = passed_along(to_prev, "cell", -1)
    cov, proj = pl.pallas_call(
        final_kernel,
        out_shape=[
            jax.ShapeDtypeStruct((mem_dev, REG_DEV, members), F32),
            jax.ShapeDtypeStruct((REG_DEV, mem_dev), F32),
        ],
        in_specs=[VMEM] * 3,
        out_specs=[VMEM] * 2,
        compiler_params=params,
        name="final",
    )(mid, from_prev, from_next)
    return (jnp.transpose(cov, (1, 0, 2)), proj)


def solution(mesh):
    in_specs = (
        P("cell", "mem", None),
        P("cell", None),
        P("cell", None),
        P("cell", None),
        P("cell", None),
        P("cell"),
        P("cell"),
        P("cell"),
    )
    out_specs = (P("cell", "mem", None), P("cell", "mem"))
    return jax.shard_map(
        on_device, mesh=mesh, in_specs=in_specs, out_specs=out_specs, check_vma=False
    )
```

```python
import jax
import jax.numpy as jnp
from jax import lax
from jax.experimental import pallas as pl
from jax.experimental.pallas import tpu as pltpu
from jax.sharding import PartitionSpec as P

REG_DEV = 8
TILE = 256
F32 = jnp.float32
BF16 = jnp.bfloat16
NT = (((1,), (1,)), ((), ()))
VMEM = pl.BlockSpec(memory_space=pltpu.VMEM)
ANY = pl.BlockSpec(memory_space=pltpu.HBM)
SMEM = pl.BlockSpec(memory_space=pltpu.SMEM)


def passed_along(x, axis, by):
    devices = lax.axis_size(axis)
    return lax.ppermute(x, axis, [(i, (i + by) % devices) for i in range(devices)])


def swapped(x, axis, mask):
    return lax.ppermute(x, axis, [(i, i ^ mask) for i in range(lax.axis_size(axis))])


def row_stride(cells):
    return cells + 4


def member_row(cells, m):
    return m * row_stride(cells) + (m >= 8)


def slot_owner(slot_ref):
    neigh, obs = slot_ref.shape
    tops = neigh * obs // 128
    o = lax.broadcasted_iota(jnp.int32, (1, obs), 1)
    upper, lower = (o >> 5).astype(F32), (o & 31).astype(F32)
    row_top = lax.broadcasted_iota(jnp.int32, (tops, obs), 0)
    row_low = lax.broadcasted_iota(jnp.int32, (128, obs), 0)
    total = jnp.zeros((2 * tops, 128), F32)
    for k in range(neigh):
        s = slot_ref[k : k + 1, :]
        hit = row_top == (s >> 7)
        lhs = jnp.concatenate(
            [jnp.where(hit, upper, 0.0), jnp.where(hit, lower, 0.0)], axis=0
        ).astype(BF16)
        rhs = jnp.where(row_low == (s & 127), 1.0, 0.0).astype(BF16)
        total += lax.dot_general(lhs, rhs, NT, preferred_element_type=F32)
    return (32.0 * total[:tops] + total[tops:]).astype(jnp.int32)


def slot_weights(inv_ref, vw_ref, tile, table_ref=None):
    levels, obs = vw_ref.shape
    key = jnp.concatenate([inv_ref[2 * tile : 2 * tile + 1, :], inv_ref[2 * tile + 1 : 2 * tile + 2, :]], axis=1)
    ids = lax.broadcasted_iota(jnp.int32, (obs, TILE), 0)
    pick = jnp.where(ids == key, 1.0, 0.0).astype(BF16)
    w = jnp.dot(vw_ref[...], pick, preferred_element_type=F32)
    extra = jnp.zeros((128 - levels, TILE), F32)
    if table_ref is not None:
        cells = table_ref[0:1, tile * TILE : (tile + 1) * TILE]
        sub = lax.broadcasted_iota(jnp.int32, (128 - levels, TILE), 0)
        extra = jnp.where(sub == 0, (cells >> 3).astype(F32), jnp.where(sub == 1, (cells & 7).astype(F32), extra))
    return jnp.concatenate([w, extra], axis=0).astype(BF16)


def ask_low_kernel(slot_hbm, table_hbm, vw_hbm, state_hbm, inv_ref, vw_ref, table_ref, state_ref, *refs):
    *out_refs, slot_ref, sems = refs
    members, levels, cells = state_hbm.shape
    pairs = [(slot_hbm, slot_ref), (vw_hbm, vw_ref), (table_hbm, table_ref)]
    for m in range(0, members, 2):
        pairs.append((state_hbm.at[pl.ds(m, 2)], state_ref.at[pl.ds(m, 2), pl.ds(0, levels), :]))
    for m in range(members):
        state_ref[m, levels:, :] = jnp.zeros((state_ref.shape[1] - levels, cells), BF16)
    copies = [pltpu.make_async_copy(src, dst, sems.at[i]) for i, (src, dst) in enumerate(pairs)]
    for copy in copies:
        copy.start()
    copies[0].wait()
    inv_ref[...] = slot_owner(slot_ref)
    copies[1].wait()
    copies[2].wait()
    halo_weights(inv_ref, vw_ref, table_ref, out_refs, (0, 1))
    for copy in copies[3:]:
        copy.wait()


def ask_high_kernel(inv_ref, vw_ref, table_ref, own_ref, *out_refs):
    halo_weights(inv_ref, vw_ref, table_ref, out_refs, (2, 3))
    for tile in range(own_ref.shape[1] // TILE):
        own_ref[:, tile * TILE : (tile + 1) * TILE] = slot_weights(inv_ref, vw_ref, tile)


def halo_weights(inv_ref, vw_ref, table_ref, out_refs, numbers):
    obs = vw_ref.shape[1]
    for out, number in zip(out_refs, numbers):
        count = out.shape[1] // TILE
        for part in range(count):
            tile = obs // TILE + number * count + part
            out[:, part * TILE : (part + 1) * TILE] = slot_weights(inv_ref, vw_ref, tile, table_ref)


def answer_tile(cell_of, w, turned_ref, cells_dim):
    S, rest = row_stride(cells_dim), member_row(cells_dim, 8)
    half = TILE // 2
    lane = lax.broadcasted_iota(jnp.int32, (8, 128), 1)
    near = lane - (lax.broadcasted_iota(jnp.int32, (8, 128), 0) >> 1)
    wide = lax.broadcasted_iota(jnp.int32, (128, TILE), 1)
    zero = jnp.zeros_like(w)
    rhs = jnp.concatenate([jnp.where(wide < half, w, zero), jnp.where(wide < half, zero, w)], axis=0)
    parts = []
    for o in range(half // 8):
        sides = []
        for h in range(2):
            a_rows, b_rows = [], []
            for j in range(8):
                c = cell_of(h * half + 8 * o + j)
                a_rows.append(turned_ref[pl.ds(c, 8, stride=S), :])
                b_rows.append(turned_ref[pl.ds(c + rest, 2, stride=S), :])
            sides.append(jnp.concatenate(a_rows + b_rows, axis=0).astype(BF16))
        parts.append(jnp.concatenate(sides, axis=1))
    d = jnp.dot(jnp.concatenate(parts, axis=0), rhs, preferred_element_type=F32)
    out_a = [jnp.zeros((8, 128), F32)] * 2
    out_b = [jnp.zeros((8, 128), F32)] * 2
    for o in range(half // 8):
        for j in range(8):
            low = 80 * o + 8 * j
            hit = lane == 8 * o + j
            for h in range(2):
                out_a[h] = jnp.where(hit, d[low : low + 8, h * half : (h + 1) * half], out_a[h])
        for i in range(2):
            low = 80 * o + 64 + 8 * i
            hit = near == 8 * o + 4 * i
            for h in range(2):
                out_b[h] = jnp.where(hit, d[low : low + 8, h * half : (h + 1) * half], out_b[h])
    return jnp.concatenate([jnp.concatenate(out_a, axis=1), jnp.concatenate(out_b, axis=1)], axis=0)


def own_kernel(state_ref, table_hbm, w_ref, turned_ref, eq_ref, cell_ref, cell_sem):
    members, levels, cells = state_ref.shape
    copy = pltpu.make_async_copy(table_hbm.at[:, pl.ds(0, eq_ref.shape[1])], cell_ref, cell_sem)
    copy.start()
    r = lax.broadcasted_iota(jnp.int32, (TILE, TILE), 0)
    eye = jnp.where(r == lax.broadcasted_iota(jnp.int32, (TILE, TILE), 1), 1.0, 0.0).astype(BF16)
    for m in range(0, members, 2):
        for part in range(cells // TILE):
            at = slice(part * TILE, (part + 1) * TILE)
            block = jnp.concatenate([state_ref[m, :, at], state_ref[m + 1, :, at]], axis=0)
            flat = lax.dot_general(eye, block, NT, preferred_element_type=F32)
            for i in range(2):
                low = member_row(cells, m + i) + part * TILE
                turned_ref[low : low + TILE, :] = flat[:, i * 128 : (i + 1) * 128]
    copy.wait()
    for tile in range(eq_ref.shape[1] // TILE):
        at = slice(tile * TILE, (tile + 1) * TILE)
        eq_ref[:, at] = answer_tile(lambda i: cell_ref[0, tile * TILE + i], w_ref[:, at], turned_ref, cells)


def answer_kernel(levels, cells, turned_ref, w_ref, before_ref, eq_ref, words, scalars, sem):
    tail = w_ref[112:128, :].astype(F32)
    row = levels - 112
    words[...] = (8.0 * tail[row : row + 1, :] + tail[row + 1 : row + 2, :]).astype(jnp.int32)
    copy = pltpu.make_async_copy(words, scalars, sem)
    copy.start()
    keep = lax.broadcasted_iota(jnp.int32, (128, TILE), 0) < levels
    copy.wait()
    for tile in range(eq_ref.shape[1] // TILE):
        at = slice(tile * TILE, (tile + 1) * TILE)
        w = w_ref[:, at]
        w = jnp.where(keep, w, jnp.zeros_like(w))
        eq_ref[:, at] = answer_tile(lambda j: scalars[0, tile * TILE + j], w, turned_ref, cells)


def combine_kernel(firsts, slot_ref, hw_ref, *refs):
    *eq_refs, out_ref = refs
    before = eq_refs.pop(0) if len(eq_refs) > len(firsts) else None
    neigh, obs = slot_ref.shape
    sub = lax.broadcasted_iota(jnp.int32, (8, 128), 0)
    tops, pairs = {}, {}
    for first, ref in zip(firsts, eq_refs):
        for part in range(ref.shape[1] // 128):
            tops[first + part] = ref[0:8, part * 128 : (part + 1) * 128]
            x = ref[8:16, part * 128 : (part + 1) * 128]
            x = x + pltpu.roll(x, 4, 0)
            pairs[first + part] = x + pltpu.roll(x, 2, 0)
    quads = {}
    for q in sorted({i // 4 for i in pairs}):
        x = jnp.zeros((8, 128), F32)
        for j in range(4):
            if 4 * q + j in pairs:
                x = jnp.where(sub >> 1 == j, pairs[4 * q + j], x)
        quads[q] = x
    last = None
    for block in range(obs // 128):
        at = slice(block * 128, (block + 1) * 128)
        a_sum = jnp.zeros((8, 128), F32)
        b_sum = jnp.zeros((8, 128), F32)
        for k in range(neigh):
            s = jnp.broadcast_to(slot_ref[k : k + 1, at], (8, 128))
            low, top = s & 127, s >> 7
            a = jnp.zeros((8, 128), F32)
            for i, x in tops.items():
                a = jnp.where(top == i, jnp.take_along_axis(x, low, axis=1, mode="promise_in_bounds"), a)
            b = jnp.zeros((8, 128), F32)
            top4 = top >> 2
            for i, x in quads.items():
                b = jnp.where(top4 == i, jnp.take_along_axis(x, low, axis=1, mode="promise_in_bounds"), b)
            b = jnp.where((top & 3) == (sub >> 1), b, 0.0)
            h = hw_ref[k : k + 1, at]
            a_sum += a * h
            b_sum += b * h
        b_sum = b_sum + pltpu.roll(b_sum, 4, 0)
        b_sum = b_sum + pltpu.roll(b_sum, 2, 0)
        if before is not None:
            a_sum += before[:, at]
        out_ref[:, at] = a_sum
        last = b_sum if block % 4 == 0 else jnp.where(sub >> 1 >= block % 4, b_sum, last)
        if block % 4 == 3:
            low = obs + block // 4 * 128
            if before is not None:
                last += before[:, low : low + 128]
            out_ref[:, low : low + 128] = last


def unpacked(ref, obs):
    sub = lax.broadcasted_iota(jnp.int32, (8, 128), 0)
    rest = []
    for block in range(obs // 128):
        low = obs + block // 4 * 128
        x = ref[:, low : low + 128]
        if block % 4:
            x = pltpu.roll(x, 8 - 2 * (block % 4), 0)
        rest.append(jnp.where(sub < 2, x, 0.0))
    return jnp.concatenate([ref[:, :obs], jnp.concatenate(rest, axis=1)], axis=0)


def split(x):
    top = x.astype(BF16)
    return top, (x - top.astype(F32)).astype(BF16)


def cov_kernel(members, own_ref, r1_ref, r2_ref, r3_ref, value_ref, error_ref, region_ref, mid_ref, prev_ref, next_ref):
    mem_dev = members // 4
    obs = region_ref.shape[1]
    blocks = [unpacked(ref, obs) for ref in (own_ref, r1_ref, r2_ref, r3_ref)]
    total = blocks[0] + blocks[1] + blocks[2] + blocks[3]
    mean = jnp.sum(total, axis=0, keepdims=True) * (1.0 / members)
    err = error_ref[...]
    inverse = 1.0 / (err * err)
    innov = (value_ref[...] - mean) * inverse
    row = lax.broadcasted_iota(jnp.int32, (16, obs), 0)
    spread = [jnp.where(row < mem_dev, x - mean, 0.0) for x in blocks]
    right = [x * inverse for x in spread]
    right[0] = jnp.where(row == mem_dev, innov, right[0])
    r_top, r_low = split(jnp.concatenate(right, axis=0))
    regions = lax.axis_size("cell") * REG_DEV
    rel = region_ref[...] - (lax.axis_index("cell") - 1) * REG_DEV
    rel = jnp.where(rel < 0, rel + regions, rel)
    rel = jnp.where(rel >= regions, rel - regions, rel)
    region = lax.broadcasted_iota(jnp.int32, (REG_DEV, obs), 0)
    own = spread[0]
    own_low = own - own.astype(BF16).astype(F32)
    for g, out_ref in ((0, prev_ref), (2, next_ref), (1, mid_ref)):
        mask = rel == region + g * REG_DEV
        l_top = jnp.concatenate([jnp.where(mask, own[m : m + 1, :], 0.0) for m in range(mem_dev)], axis=0).astype(BF16)
        l_low = jnp.concatenate([jnp.where(mask, own_low[m : m + 1, :], 0.0) for m in range(mem_dev)], axis=0).astype(BF16)
        d = lax.dot_general(l_top, r_top, NT, preferred_element_type=F32)
        d += lax.dot_general(l_top, r_low, NT, preferred_element_type=F32)
        d += lax.dot_general(l_low, r_top, NT, preferred_element_type=F32)
        out_ref[...] = d


def final_kernel(mid_ref, a_ref, b_ref, cov_ref, proj_ref):
    mem_dev, regions, members = cov_ref.shape
    d = mid_ref[...] + a_ref[...] + b_ref[...]
    width = d.shape[1]
    i = lax.broadcasted_iota(jnp.int32, (width, members), 0)
    j = lax.broadcasted_iota(jnp.int32, (width, members), 1)
    block = lax.axis_index("mem") ^ (i >> 4)
    place = jnp.where(((i & 15) < mem_dev) & (block * mem_dev + (i & 15) == j), 1.0, 0.0)
    cov = jnp.dot(d, place, precision=lax.Precision.HIGHEST, preferred_element_type=F32)
    lane = lax.broadcasted_iota(jnp.int32, (regions, mem_dev), 1)
    proj = jnp.zeros((regions, mem_dev), F32)
    for m in range(mem_dev):
        cov_ref[m] = cov[m * regions : (m + 1) * regions, :]
        proj = jnp.where(lane == m, d[m * regions : (m + 1) * regions, mem_dev : mem_dev + 1], proj)
    proj_ref[...] = proj


def on_device(state, vertical_weight, horizontal_weight, obs_slot, request_cell, obs_value, obs_error, obs_region):
    cells, mem_dev, levels = state.shape
    members = mem_dev * lax.axis_size("mem")
    obs, neigh = obs_slot.shape
    halo = 3 * obs // 4
    state_t = jnp.transpose(state, (1, 2, 0))
    vw_t, hw_t, slot_t = vertical_weight.T, horizontal_weight.T, obs_slot.T
    far = lambda x: pltpu.with_memory_space_constraint(x, pltpu.HBM)
    params = pltpu.CompilerParams(vmem_limit_bytes=16 * 1024 * 1024)

    w_shape = jax.ShapeDtypeStruct((128, halo), BF16)
    inv, vw_near, table, state_near, ask_m2, ask_m1 = pl.pallas_call(
        ask_low_kernel,
        out_shape=[
            pltpu.VMEM((neigh * obs // 128, 128), jnp.int32),
            pltpu.VMEM((levels, obs), BF16),
            pltpu.VMEM((1, neigh * obs), jnp.int32),
            pltpu.VMEM((mem_dev, 128, cells), BF16),
            w_shape,
            w_shape,
        ],
        in_specs=[ANY] * 4,
        out_specs=[VMEM] * 6,
        scratch_shapes=[pltpu.VMEM((neigh, obs), jnp.int32), pltpu.SemaphoreType.DMA((3 + mem_dev // 2,))],
        compiler_params=params,
        cost_estimate=pl.CostEstimate(flops=2_000_000_000, bytes_accessed=6_000_000, transcendentals=0),
        name="ask_low",
    )(far(slot_t), far(request_cell), far(vw_t), far(state_t))
    w_m2, w_m1 = passed_along(ask_m2, "cell", -2), passed_along(ask_m1, "cell", -1)
    w_own, ask_p1, ask_p2 = pl.pallas_call(
        ask_high_kernel,
        out_shape=[pltpu.VMEM((128, obs), BF16), w_shape, w_shape],
        in_specs=[VMEM] * 3,
        out_specs=[VMEM] * 3,
        compiler_params=params,
        cost_estimate=pl.CostEstimate(flops=2_000_000_000, bytes_accessed=1_000_000, transcendentals=0),
        name="ask_high",
    )(inv, vw_near, table)
    w_p1, w_p2 = passed_along(ask_p1, "cell", 1), passed_along(ask_p2, "cell", 2)
    turned, eq_own = pl.pallas_call(
        own_kernel,
        out_shape=[
            pltpu.VMEM((mem_dev * row_stride(cells), 128), F32),
            pltpu.VMEM((16, obs), F32),
        ],
        in_specs=[VMEM, ANY, VMEM],
        out_specs=[VMEM] * 2,
        scratch_shapes=[pltpu.SMEM((1, obs), jnp.int32), pltpu.SemaphoreType.DMA],
        compiler_params=params,
        cost_estimate=pl.CostEstimate(flops=8_000_000_000, bytes_accessed=10_000_000, transcendentals=0),
        name="own",
    )(state_near, far(request_cell), w_own)
    turned = pltpu.with_memory_space_constraint(turned, pltpu.VMEM)
    answer = pl.pallas_call(
        lambda *refs: answer_kernel(levels, cells, *refs),
        out_shape=pltpu.VMEM((16, halo), F32),
        in_specs=[VMEM] * 3,
        out_specs=VMEM,
        scratch_shapes=[
            pltpu.VMEM((1, halo), jnp.int32),
            pltpu.SMEM((1, halo), jnp.int32),
            pltpu.SemaphoreType.DMA,
        ],
        compiler_params=params,
        cost_estimate=pl.CostEstimate(flops=2_000_000_000, bytes_accessed=1_000_000, transcendentals=0),
        name="answer",
    )
    sent_m2 = answer(turned, w_m2, eq_own)
    eq_m2 = passed_along(sent_m2, "cell", 2)
    sent_m1 = answer(turned, w_m1, sent_m2)
    eq_m1 = passed_along(sent_m1, "cell", 1)
    sent_p1 = answer(turned, w_p1, sent_m1)
    eq_p1 = passed_along(sent_p1, "cell", -1)
    sent_p2 = answer(turned, w_p2, sent_p1)
    eq_p2 = passed_along(sent_p2, "cell", -2)

    def combine(tables, *before):
        firsts = [obs // 128 + n * halo // 128 if n >= 0 else 0 for n, _ in tables]
        return pl.pallas_call(
            lambda *refs: combine_kernel(firsts, *refs),
            out_shape=jax.ShapeDtypeStruct((8, obs + obs // 4), F32),
            in_specs=[VMEM] * (2 + len(before) + len(tables)),
            out_specs=VMEM,
            compiler_params=params,
            cost_estimate=pl.CostEstimate(flops=1_000_000_000, bytes_accessed=1_000_000, transcendentals=0),
            name="combine",
        )(slot_t, hw_t, *before, *(x for _, x in tables))

    own = combine([(-1, eq_own), (0, eq_m2), (1, eq_m1)])
    own = combine([(2, eq_p1), (3, eq_p2)], own)
    others = [swapped(own, "mem", mask) for mask in (1, 2, 3)]
    wide = 4 * 16
    mid, to_prev, to_next = pl.pallas_call(
        lambda *refs: cov_kernel(members, *refs),
        out_shape=[jax.ShapeDtypeStruct((mem_dev * REG_DEV, wide), F32)] * 3,
        in_specs=[VMEM] * 7,
        out_specs=[VMEM] * 3,
        compiler_params=params,
        name="cov",
    )(own, *others, obs_value.reshape(1, obs), obs_error.reshape(1, obs), obs_region.reshape(1, obs))
    from_prev = passed_along(to_next, "cell", 1)
    from_next = passed_along(to_prev, "cell", -1)
    cov, proj = pl.pallas_call(
        final_kernel,
        out_shape=[
            jax.ShapeDtypeStruct((mem_dev, REG_DEV, members), F32),
            jax.ShapeDtypeStruct((REG_DEV, mem_dev), F32),
        ],
        in_specs=[VMEM] * 3,
        out_specs=[VMEM] * 2,
        compiler_params=params,
        name="final",
    )(mid, from_prev, from_next)
    return (jnp.transpose(cov, (1, 0, 2)), proj)


def solution(mesh):
    in_specs = (
        P("cell", "mem", None),
        P("cell", None),
        P("cell", None),
        P("cell", None),
        P("cell", None),
        P("cell"),
        P("cell"),
        P("cell"),
    )
    out_specs = (P("cell", "mem", None), P("cell", "mem"))
    return jax.shard_map(
        on_device, mesh=mesh, in_specs=in_specs, out_specs=out_specs, check_vma=False
    )
```

```python
import jax
import jax.numpy as jnp
from jax import lax
from jax.experimental import pallas as pl
from jax.experimental.pallas import tpu as pltpu
from jax.sharding import PartitionSpec as P

REG_DEV = 8
TILE = 256
F32 = jnp.float32
BF16 = jnp.bfloat16
NT = (((1,), (1,)), ((), ()))
VMEM = pl.BlockSpec(memory_space=pltpu.VMEM)
ANY = pl.BlockSpec(memory_space=pltpu.HBM)
SMEM = pl.BlockSpec(memory_space=pltpu.SMEM)


def passed_along(x, axis, by):
    devices = lax.axis_size(axis)
    return lax.ppermute(x, axis, [(i, (i + by) % devices) for i in range(devices)])


def swapped(x, axis, mask):
    return lax.ppermute(x, axis, [(i, i ^ mask) for i in range(lax.axis_size(axis))])


def row_stride(cells):
    return cells + 4


def member_row(cells, m):
    return m * row_stride(cells) + (m >= 8)


def slot_owner(slot_ref):
    neigh, obs = slot_ref.shape
    tops = neigh * obs // 128
    o = lax.broadcasted_iota(jnp.int32, (1, obs), 1)
    upper, lower = (o >> 5).astype(F32), (o & 31).astype(F32)
    row_top = lax.broadcasted_iota(jnp.int32, (tops, obs), 0)
    row_low = lax.broadcasted_iota(jnp.int32, (128, obs), 0)
    total = jnp.zeros((2 * tops, 128), F32)
    for k in range(neigh):
        s = slot_ref[k : k + 1, :]
        hit = row_top == (s >> 7)
        lhs = jnp.concatenate(
            [jnp.where(hit, upper, 0.0), jnp.where(hit, lower, 0.0)], axis=0
        ).astype(BF16)
        rhs = jnp.where(row_low == (s & 127), 1.0, 0.0).astype(BF16)
        total += lax.dot_general(lhs, rhs, NT, preferred_element_type=F32)
    return (32.0 * total[:tops] + total[tops:]).astype(jnp.int32)


def slot_weights(inv_ref, vw_ref, tile, table_ref=None):
    levels, obs = vw_ref.shape
    key = jnp.concatenate([inv_ref[2 * tile : 2 * tile + 1, :], inv_ref[2 * tile + 1 : 2 * tile + 2, :]], axis=1)
    ids = lax.broadcasted_iota(jnp.int32, (obs, TILE), 0)
    pick = jnp.where(ids == key, 1.0, 0.0).astype(BF16)
    w = jnp.dot(vw_ref[...], pick, preferred_element_type=F32)
    extra = jnp.zeros((128 - levels, TILE), F32)
    if table_ref is not None:
        cells = table_ref[0:1, tile * TILE : (tile + 1) * TILE]
        sub = lax.broadcasted_iota(jnp.int32, (128 - levels, TILE), 0)
        extra = jnp.where(sub == 0, (cells >> 3).astype(F32), jnp.where(sub == 1, (cells & 7).astype(F32), extra))
    return jnp.concatenate([w, extra], axis=0).astype(BF16)


def ask_low_kernel(slot_hbm, table_hbm, vw_hbm, state_hbm, inv_ref, vw_ref, table_ref, state_ref, *refs):
    *out_refs, slot_ref, sems = refs
    members, levels, cells = state_hbm.shape
    pairs = [(slot_hbm, slot_ref), (vw_hbm, vw_ref), (table_hbm, table_ref)]
    for m in range(0, members, 2):
        pairs.append((state_hbm.at[pl.ds(m, 2)], state_ref.at[pl.ds(m, 2), pl.ds(0, levels), :]))
    for m in range(members):
        state_ref[m, levels:, :] = jnp.zeros((state_ref.shape[1] - levels, cells), BF16)
    copies = [pltpu.make_async_copy(src, dst, sems.at[i]) for i, (src, dst) in enumerate(pairs)]
    for copy in copies:
        copy.start()
    copies[0].wait()
    inv_ref[...] = slot_owner(slot_ref)
    copies[1].wait()
    copies[2].wait()
    halo_weights(inv_ref, vw_ref, table_ref, out_refs, (0, 1))
    for copy in copies[3:]:
        copy.wait()


def ask_high_kernel(inv_ref, vw_ref, table_ref, own_ref, *out_refs):
    halo_weights(inv_ref, vw_ref, table_ref, out_refs, (2, 3))
    for tile in range(own_ref.shape[1] // TILE):
        own_ref[:, tile * TILE : (tile + 1) * TILE] = slot_weights(inv_ref, vw_ref, tile)


def halo_weights(inv_ref, vw_ref, table_ref, out_refs, numbers):
    obs = vw_ref.shape[1]
    for out, number in zip(out_refs, numbers):
        count = out.shape[1] // TILE
        for part in range(count):
            tile = obs // TILE + number * count + part
            out[:, part * TILE : (part + 1) * TILE] = slot_weights(inv_ref, vw_ref, tile, table_ref)


def answer_tile(cell_of, w, turned_ref, cells_dim):
    S, rest = row_stride(cells_dim), member_row(cells_dim, 8)
    half = TILE // 2
    lane = lax.broadcasted_iota(jnp.int32, (8, 128), 1)
    near = lane - (lax.broadcasted_iota(jnp.int32, (8, 128), 0) >> 1)
    wide = lax.broadcasted_iota(jnp.int32, (128, TILE), 1)
    zero = jnp.zeros_like(w)
    rhs = jnp.concatenate([jnp.where(wide < half, w, zero), jnp.where(wide < half, zero, w)], axis=0)
    parts = []
    for o in range(half // 8):
        sides = []
        for h in range(2):
            a_rows, b_rows = [], []
            for j in range(8):
                c = cell_of(h * half + 8 * o + j)
                a_rows.append(turned_ref[pl.ds(c, 8, stride=S), :])
                b_rows.append(turned_ref[pl.ds(c + rest, 2, stride=S), :])
            sides.append(jnp.concatenate(a_rows + b_rows, axis=0).astype(BF16))
        parts.append(jnp.concatenate(sides, axis=1))
    d = jnp.dot(jnp.concatenate(parts, axis=0), rhs, preferred_element_type=F32)
    out_a = [jnp.zeros((8, 128), F32)] * 2
    out_b = [jnp.zeros((8, 128), F32)] * 2
    for o in range(half // 8):
        for j in range(8):
            low = 80 * o + 8 * j
            hit = lane == 8 * o + j
            for h in range(2):
                out_a[h] = jnp.where(hit, d[low : low + 8, h * half : (h + 1) * half], out_a[h])
        for i in range(2):
            low = 80 * o + 64 + 8 * i
            hit = near == 8 * o + 4 * i
            for h in range(2):
                out_b[h] = jnp.where(hit, d[low : low + 8, h * half : (h + 1) * half], out_b[h])
    return jnp.concatenate([jnp.concatenate(out_a, axis=1), jnp.concatenate(out_b, axis=1)], axis=0)


def own_kernel(state_ref, table_hbm, w_ref, turned_ref, eq_ref, cell_ref, cell_sem):
    members, levels, cells = state_ref.shape
    copy = pltpu.make_async_copy(table_hbm.at[:, pl.ds(0, eq_ref.shape[1])], cell_ref, cell_sem)
    copy.start()
    r = lax.broadcasted_iota(jnp.int32, (TILE, TILE), 0)
    eye = jnp.where(r == lax.broadcasted_iota(jnp.int32, (TILE, TILE), 1), 1.0, 0.0).astype(BF16)
    for m in range(0, members, 2):
        for part in range(cells // TILE):
            at = slice(part * TILE, (part + 1) * TILE)
            block = jnp.concatenate([state_ref[m, :, at], state_ref[m + 1, :, at]], axis=0)
            flat = lax.dot_general(eye, block, NT, preferred_element_type=F32)
            for i in range(2):
                low = member_row(cells, m + i) + part * TILE
                turned_ref[low : low + TILE, :] = flat[:, i * 128 : (i + 1) * 128]
    copy.wait()
    for tile in range(eq_ref.shape[1] // TILE):
        at = slice(tile * TILE, (tile + 1) * TILE)
        eq_ref[:, at] = answer_tile(lambda i: cell_ref[0, tile * TILE + i], w_ref[:, at], turned_ref, cells)


def answer_kernel(levels, cells, turned_ref, w_ref, before_ref, eq_ref):
    tail = w_ref[112:128, :].astype(F32)
    row = levels - 112
    words = (8.0 * tail[row : row + 1, :] + tail[row + 1 : row + 2, :]).astype(jnp.int32)
    keep = lax.broadcasted_iota(jnp.int32, (128, TILE), 0) < levels
    for tile in range(eq_ref.shape[1] // TILE):
        at = slice(tile * TILE, (tile + 1) * TILE)
        w = w_ref[:, at]
        w = jnp.where(keep, w, jnp.zeros_like(w))
        eq_ref[:, at] = answer_tile(lambda j: words[0, tile * TILE + j], w, turned_ref, cells)


def combine_kernel(firsts, slot_ref, hw_ref, *refs):
    *eq_refs, out_ref = refs
    before = eq_refs.pop(0) if len(eq_refs) > len(firsts) else None
    neigh, obs = slot_ref.shape
    sub = lax.broadcasted_iota(jnp.int32, (8, 128), 0)
    tops, pairs = {}, {}
    for first, ref in zip(firsts, eq_refs):
        for part in range(ref.shape[1] // 128):
            tops[first + part] = ref[0:8, part * 128 : (part + 1) * 128]
            x = ref[8:16, part * 128 : (part + 1) * 128]
            x = x + pltpu.roll(x, 4, 0)
            pairs[first + part] = x + pltpu.roll(x, 2, 0)
    quads = {}
    for q in sorted({i // 4 for i in pairs}):
        x = jnp.zeros((8, 128), F32)
        for j in range(4):
            if 4 * q + j in pairs:
                x = jnp.where(sub >> 1 == j, pairs[4 * q + j], x)
        quads[q] = x
    last = None
    for block in range(obs // 128):
        at = slice(block * 128, (block + 1) * 128)
        a_sum = jnp.zeros((8, 128), F32)
        b_sum = jnp.zeros((8, 128), F32)
        for k in range(neigh):
            s = jnp.broadcast_to(slot_ref[k : k + 1, at], (8, 128))
            low, top = s & 127, s >> 7
            a = jnp.zeros((8, 128), F32)
            for i, x in tops.items():
                a = jnp.where(top == i, jnp.take_along_axis(x, low, axis=1, mode="promise_in_bounds"), a)
            b = jnp.zeros((8, 128), F32)
            top4 = top >> 2
            for i, x in quads.items():
                b = jnp.where(top4 == i, jnp.take_along_axis(x, low, axis=1, mode="promise_in_bounds"), b)
            b = jnp.where((top & 3) == (sub >> 1), b, 0.0)
            h = hw_ref[k : k + 1, at]
            a_sum += a * h
            b_sum += b * h
        b_sum = b_sum + pltpu.roll(b_sum, 4, 0)
        b_sum = b_sum + pltpu.roll(b_sum, 2, 0)
        if before is not None:
            a_sum += before[:, at]
        out_ref[:, at] = a_sum
        last = b_sum if block % 4 == 0 else jnp.where(sub >> 1 >= block % 4, b_sum, last)
        if block % 4 == 3:
            low = obs + block // 4 * 128
            if before is not None:
                last += before[:, low : low + 128]
            out_ref[:, low : low + 128] = last


def unpacked(ref, obs):
    sub = lax.broadcasted_iota(jnp.int32, (8, 128), 0)
    rest = []
    for block in range(obs // 128):
        low = obs + block // 4 * 128
        x = ref[:, low : low + 128]
        if block % 4:
            x = pltpu.roll(x, 8 - 2 * (block % 4), 0)
        rest.append(jnp.where(sub < 2, x, 0.0))
    return jnp.concatenate([ref[:, :obs], jnp.concatenate(rest, axis=1)], axis=0)


def split(x):
    top = x.astype(BF16)
    return top, (x - top.astype(F32)).astype(BF16)


def cov_kernel(members, own_ref, r1_ref, r2_ref, r3_ref, value_ref, error_ref, region_ref, mid_ref, prev_ref, next_ref):
    mem_dev = members // 4
    obs = region_ref.shape[1]
    blocks = [unpacked(ref, obs) for ref in (own_ref, r1_ref, r2_ref, r3_ref)]
    total = blocks[0] + blocks[1] + blocks[2] + blocks[3]
    mean = jnp.sum(total, axis=0, keepdims=True) * (1.0 / members)
    err = error_ref[...]
    inverse = 1.0 / (err * err)
    innov = (value_ref[...] - mean) * inverse
    row = lax.broadcasted_iota(jnp.int32, (16, obs), 0)
    spread = [jnp.where(row < mem_dev, x - mean, 0.0) for x in blocks]
    right = [x * inverse for x in spread]
    right[0] = jnp.where(row == mem_dev, innov, right[0])
    r_top, r_low = split(jnp.concatenate(right, axis=0))
    regions = lax.axis_size("cell") * REG_DEV
    rel = region_ref[...] - (lax.axis_index("cell") - 1) * REG_DEV
    rel = jnp.where(rel < 0, rel + regions, rel)
    rel = jnp.where(rel >= regions, rel - regions, rel)
    region = lax.broadcasted_iota(jnp.int32, (REG_DEV, obs), 0)
    own = spread[0]
    own_low = own - own.astype(BF16).astype(F32)
    for g, out_ref in ((0, prev_ref), (2, next_ref), (1, mid_ref)):
        mask = rel == region + g * REG_DEV
        l_top = jnp.concatenate([jnp.where(mask, own[m : m + 1, :], 0.0) for m in range(mem_dev)], axis=0).astype(BF16)
        l_low = jnp.concatenate([jnp.where(mask, own_low[m : m + 1, :], 0.0) for m in range(mem_dev)], axis=0).astype(BF16)
        d = lax.dot_general(l_top, r_top, NT, preferred_element_type=F32)
        d += lax.dot_general(l_top, r_low, NT, preferred_element_type=F32)
        d += lax.dot_general(l_low, r_top, NT, preferred_element_type=F32)
        out_ref[...] = d


def final_kernel(mid_ref, a_ref, b_ref, cov_ref, proj_ref):
    mem_dev, regions, members = cov_ref.shape
    d = mid_ref[...] + a_ref[...] + b_ref[...]
    width = d.shape[1]
    i = lax.broadcasted_iota(jnp.int32, (width, members), 0)
    j = lax.broadcasted_iota(jnp.int32, (width, members), 1)
    block = lax.axis_index("mem") ^ (i >> 4)
    place = jnp.where(((i & 15) < mem_dev) & (block * mem_dev + (i & 15) == j), 1.0, 0.0)
    cov = jnp.dot(d, place, precision=lax.Precision.HIGHEST, preferred_element_type=F32)
    lane = lax.broadcasted_iota(jnp.int32, (regions, mem_dev), 1)
    proj = jnp.zeros((regions, mem_dev), F32)
    for m in range(mem_dev):
        cov_ref[m] = cov[m * regions : (m + 1) * regions, :]
        proj = jnp.where(lane == m, d[m * regions : (m + 1) * regions, mem_dev : mem_dev + 1], proj)
    proj_ref[...] = proj


def on_device(state, vertical_weight, horizontal_weight, obs_slot, request_cell, obs_value, obs_error, obs_region):
    cells, mem_dev, levels = state.shape
    members = mem_dev * lax.axis_size("mem")
    obs, neigh = obs_slot.shape
    halo = 3 * obs // 4
    state_t = jnp.transpose(state, (1, 2, 0))
    vw_t, hw_t, slot_t = vertical_weight.T, horizontal_weight.T, obs_slot.T
    far = lambda x: pltpu.with_memory_space_constraint(x, pltpu.HBM)
    params = pltpu.CompilerParams(vmem_limit_bytes=16 * 1024 * 1024)

    w_shape = jax.ShapeDtypeStruct((128, halo), BF16)
    inv, vw_near, table, state_near, ask_m2, ask_m1 = pl.pallas_call(
        ask_low_kernel,
        out_shape=[
            pltpu.VMEM((neigh * obs // 128, 128), jnp.int32),
            pltpu.VMEM((levels, obs), BF16),
            pltpu.VMEM((1, neigh * obs), jnp.int32),
            pltpu.VMEM((mem_dev, 128, cells), BF16),
            w_shape,
            w_shape,
        ],
        in_specs=[ANY] * 4,
        out_specs=[VMEM] * 6,
        scratch_shapes=[pltpu.VMEM((neigh, obs), jnp.int32), pltpu.SemaphoreType.DMA((3 + mem_dev // 2,))],
        compiler_params=params,
        cost_estimate=pl.CostEstimate(flops=2_000_000_000, bytes_accessed=6_000_000, transcendentals=0),
        name="ask_low",
    )(far(slot_t), far(request_cell), far(vw_t), far(state_t))
    w_m2, w_m1 = passed_along(ask_m2, "cell", -2), passed_along(ask_m1, "cell", -1)
    w_own, ask_p1, ask_p2 = pl.pallas_call(
        ask_high_kernel,
        out_shape=[pltpu.VMEM((128, obs), BF16), w_shape, w_shape],
        in_specs=[VMEM] * 3,
        out_specs=[VMEM] * 3,
        compiler_params=params,
        cost_estimate=pl.CostEstimate(flops=2_000_000_000, bytes_accessed=1_000_000, transcendentals=0),
        name="ask_high",
    )(inv, vw_near, table)
    w_p1, w_p2 = passed_along(ask_p1, "cell", 1), passed_along(ask_p2, "cell", 2)
    turned, eq_own = pl.pallas_call(
        own_kernel,
        out_shape=[
            pltpu.VMEM((mem_dev * row_stride(cells), 128), F32),
            pltpu.VMEM((16, obs), F32),
        ],
        in_specs=[VMEM, ANY, VMEM],
        out_specs=[VMEM] * 2,
        scratch_shapes=[pltpu.SMEM((1, obs), jnp.int32), pltpu.SemaphoreType.DMA],
        compiler_params=params,
        cost_estimate=pl.CostEstimate(flops=8_000_000_000, bytes_accessed=10_000_000, transcendentals=0),
        name="own",
    )(state_near, far(request_cell), w_own)
    turned = pltpu.with_memory_space_constraint(turned, pltpu.VMEM)
    answer = pl.pallas_call(
        lambda *refs: answer_kernel(levels, cells, *refs),
        out_shape=pltpu.VMEM((16, halo), F32),
        in_specs=[VMEM] * 3,
        out_specs=VMEM,
        compiler_params=params,
        cost_estimate=pl.CostEstimate(flops=2_000_000_000, bytes_accessed=1_000_000, transcendentals=0),
        name="answer",
    )
    sent_m2 = answer(turned, w_m2, eq_own)
    eq_m2 = passed_along(sent_m2, "cell", 2)
    sent_m1 = answer(turned, w_m1, sent_m2)
    eq_m1 = passed_along(sent_m1, "cell", 1)
    sent_p1 = answer(turned, w_p1, sent_m1)
    eq_p1 = passed_along(sent_p1, "cell", -1)
    sent_p2 = answer(turned, w_p2, sent_p1)
    eq_p2 = passed_along(sent_p2, "cell", -2)

    def combine(tables, *before):
        firsts = [obs // 128 + n * halo // 128 if n >= 0 else 0 for n, _ in tables]
        return pl.pallas_call(
            lambda *refs: combine_kernel(firsts, *refs),
            out_shape=jax.ShapeDtypeStruct((8, obs + obs // 4), F32),
            in_specs=[VMEM] * (2 + len(before) + len(tables)),
            out_specs=VMEM,
            compiler_params=params,
            cost_estimate=pl.CostEstimate(flops=1_000_000_000, bytes_accessed=1_000_000, transcendentals=0),
            name="combine",
        )(slot_t, hw_t, *before, *(x for _, x in tables))

    own = combine([(-1, eq_own), (0, eq_m2), (1, eq_m1)])
    own = combine([(2, eq_p1), (3, eq_p2)], own)
    others = [swapped(own, "mem", mask) for mask in (1, 2, 3)]
    wide = 4 * 16
    mid, to_prev, to_next = pl.pallas_call(
        lambda *refs: cov_kernel(members, *refs),
        out_shape=[jax.ShapeDtypeStruct((mem_dev * REG_DEV, wide), F32)] * 3,
        in_specs=[VMEM] * 7,
        out_specs=[VMEM] * 3,
        compiler_params=params,
        name="cov",
    )(own, *others, obs_value.reshape(1, obs), obs_error.reshape(1, obs), obs_region.reshape(1, obs))
    from_prev = passed_along(to_next, "cell", 1)
    from_next = passed_along(to_prev, "cell", -1)
    cov, proj = pl.pallas_call(
        final_kernel,
        out_shape=[
            jax.ShapeDtypeStruct((mem_dev, REG_DEV, members), F32),
            jax.ShapeDtypeStruct((REG_DEV, mem_dev), F32),
        ],
        in_specs=[VMEM] * 3,
        out_specs=[VMEM] * 2,
        compiler_params=params,
        name="final",
    )(mid, from_prev, from_next)
    return (jnp.transpose(cov, (1, 0, 2)), proj)


def solution(mesh):
    in_specs = (
        P("cell", "mem", None),
        P("cell", None),
        P("cell", None),
        P("cell", None),
        P("cell", None),
        P("cell"),
        P("cell"),
        P("cell"),
    )
    out_specs = (P("cell", "mem", None), P("cell", "mem"))
    return jax.shard_map(
        on_device, mesh=mesh, in_specs=in_specs, out_specs=out_specs, check_vma=False
    )
```

```python
import jax
import jax.numpy as jnp
from jax import lax
from jax.experimental import pallas as pl
from jax.experimental.pallas import tpu as pltpu
from jax.sharding import PartitionSpec as P

REG_DEV = 8
TILE = 256
F32 = jnp.float32
BF16 = jnp.bfloat16
NT = (((1,), (1,)), ((), ()))
VMEM = pl.BlockSpec(memory_space=pltpu.VMEM)
ANY = pl.BlockSpec(memory_space=pltpu.HBM)
SMEM = pl.BlockSpec(memory_space=pltpu.SMEM)


def passed_along(x, axis, by):
    devices = lax.axis_size(axis)
    return lax.ppermute(x, axis, [(i, (i + by) % devices) for i in range(devices)])


def swapped(x, axis, mask):
    return lax.ppermute(x, axis, [(i, i ^ mask) for i in range(lax.axis_size(axis))])


def row_stride(cells):
    return cells + 4


def member_row(cells, m):
    return m * row_stride(cells) + (m >= 8)


def slot_owner(slot_ref):
    neigh, obs = slot_ref.shape
    tops = neigh * obs // 128
    o = lax.broadcasted_iota(jnp.int32, (1, obs), 1)
    upper, lower = (o >> 5).astype(F32), (o & 31).astype(F32)
    row_top = lax.broadcasted_iota(jnp.int32, (tops, obs), 0)
    row_low = lax.broadcasted_iota(jnp.int32, (128, obs), 0)
    total = jnp.zeros((2 * tops, 128), F32)
    for k in range(neigh):
        s = slot_ref[k : k + 1, :]
        hit = row_top == (s >> 7)
        lhs = jnp.concatenate(
            [jnp.where(hit, upper, 0.0), jnp.where(hit, lower, 0.0)], axis=0
        ).astype(BF16)
        rhs = jnp.where(row_low == (s & 127), 1.0, 0.0).astype(BF16)
        total += lax.dot_general(lhs, rhs, NT, preferred_element_type=F32)
    return (32.0 * total[:tops] + total[tops:]).astype(jnp.int32)


def slot_weights(inv_ref, vw_ref, tile, table_ref=None):
    levels, obs = vw_ref.shape
    key = jnp.concatenate([inv_ref[2 * tile : 2 * tile + 1, :], inv_ref[2 * tile + 1 : 2 * tile + 2, :]], axis=1)
    ids = lax.broadcasted_iota(jnp.int32, (obs, TILE), 0)
    pick = jnp.where(ids == key, 1.0, 0.0).astype(BF16)
    w = jnp.dot(vw_ref[...], pick, preferred_element_type=F32)
    extra = jnp.zeros((128 - levels, TILE), F32)
    if table_ref is not None:
        cells = table_ref[0:1, tile * TILE : (tile + 1) * TILE]
        sub = lax.broadcasted_iota(jnp.int32, (128 - levels, TILE), 0)
        extra = jnp.where(sub == 0, (cells >> 3).astype(F32), jnp.where(sub == 1, (cells & 7).astype(F32), extra))
    return jnp.concatenate([w, extra], axis=0).astype(BF16)


def ask_low_kernel(slot_hbm, table_hbm, vw_hbm, state_hbm, inv_ref, vw_ref, table_ref, state_ref, *refs):
    *out_refs, slot_ref, sems = refs
    levels, cells = state_hbm.shape[1:]
    members = state_ref.shape[0]
    pairs = [(slot_hbm, slot_ref), (vw_hbm, vw_ref), (table_hbm, table_ref)]
    for m in range(0, members, 2):
        pairs.append((state_hbm.at[pl.ds(m, 2)], state_ref.at[pl.ds(m, 2), pl.ds(0, levels), :]))
    for m in range(members):
        state_ref[m, levels:, :] = jnp.zeros((state_ref.shape[1] - levels, cells), BF16)
    copies = [pltpu.make_async_copy(src, dst, sems.at[i]) for i, (src, dst) in enumerate(pairs)]
    for copy in copies:
        copy.start()
    copies[0].wait()
    inv_ref[...] = slot_owner(slot_ref)
    copies[1].wait()
    copies[2].wait()
    halo_weights(inv_ref, vw_ref, table_ref, out_refs, (0, 1))
    for copy in copies[3:]:
        copy.wait()


def ask_high_kernel(inv_ref, vw_ref, table_ref, own_ref, *out_refs):
    halo_weights(inv_ref, vw_ref, table_ref, out_refs, (2, 3))
    for tile in range(own_ref.shape[1] // TILE):
        own_ref[:, tile * TILE : (tile + 1) * TILE] = slot_weights(inv_ref, vw_ref, tile)


def halo_weights(inv_ref, vw_ref, table_ref, out_refs, numbers):
    obs = vw_ref.shape[1]
    for out, number in zip(out_refs, numbers):
        count = out.shape[1] // TILE
        for part in range(count):
            tile = obs // TILE + number * count + part
            out[:, part * TILE : (part + 1) * TILE] = slot_weights(inv_ref, vw_ref, tile, table_ref)


def answer_tile(pair_of, w, turned_ref, cells_dim):
    S, rest = row_stride(cells_dim), member_row(cells_dim, 8)
    half = TILE // 2
    lane = lax.broadcasted_iota(jnp.int32, (8, 128), 1)
    near = lane - (lax.broadcasted_iota(jnp.int32, (8, 128), 0) >> 1)
    wide = lax.broadcasted_iota(jnp.int32, (128, TILE), 1)
    zero = jnp.zeros_like(w)
    rhs = jnp.concatenate([jnp.where(wide < half, w, zero), jnp.where(wide < half, zero, w)], axis=0)
    parts = []
    for o in range(half // 8):
        sides = []
        pairs = [pair_of(8 * o + j) for j in range(8)]
        for h in range(2):
            a_rows, b_rows = [], []
            for j in range(8):
                c = pairs[j][h]
                a_rows.append(turned_ref[pl.ds(c, 8, stride=S), :])
                b_rows.append(turned_ref[pl.ds(c + rest, 2, stride=S), :])
            sides.append(jnp.concatenate(a_rows + b_rows, axis=0).astype(BF16))
        parts.append(jnp.concatenate(sides, axis=1))
    d = jnp.dot(jnp.concatenate(parts, axis=0), rhs, preferred_element_type=F32)
    out_a = [jnp.zeros((8, 128), F32)] * 2
    out_b = [jnp.zeros((8, 128), F32)] * 2
    for o in range(half // 8):
        for j in range(8):
            low = 80 * o + 8 * j
            hit = lane == 8 * o + j
            for h in range(2):
                out_a[h] = jnp.where(hit, d[low : low + 8, h * half : (h + 1) * half], out_a[h])
        for i in range(2):
            low = 80 * o + 64 + 8 * i
            hit = near == 8 * o + 4 * i
            for h in range(2):
                out_b[h] = jnp.where(hit, d[low : low + 8, h * half : (h + 1) * half], out_b[h])
    return jnp.concatenate([jnp.concatenate(out_a, axis=1), jnp.concatenate(out_b, axis=1)], axis=0)


def own_kernel(first_ref, state_hbm, table_hbm, w_ref, turned_ref, eq_ref, rest_ref, cell_ref, cell_sem, sems):
    members, levels, cells = state_hbm.shape
    early = first_ref.shape[0]
    for m in range(members - early):
        rest_ref[m, levels:, :] = jnp.zeros((rest_ref.shape[1] - levels, cells), BF16)
    late = [
        pltpu.make_async_copy(
            state_hbm.at[pl.ds(m, 2)], rest_ref.at[pl.ds(m - early, 2), pl.ds(0, levels), :], sems.at[(m - early) // 2]
        )
        for m in range(early, members, 2)
    ]
    for each in late:
        each.start()
    copy = pltpu.make_async_copy(table_hbm.at[:, pl.ds(0, eq_ref.shape[1])], cell_ref, cell_sem)
    copy.start()
    r = lax.broadcasted_iota(jnp.int32, (TILE, TILE), 0)
    eye = jnp.where(r == lax.broadcasted_iota(jnp.int32, (TILE, TILE), 1), 1.0, 0.0).astype(BF16)
    for m in range(0, members, 2):
        state_ref, n = (first_ref, m) if m < early else (rest_ref, m - early)
        if m >= early:
            late[n // 2].wait()
        for part in range(cells // TILE):
            at = slice(part * TILE, (part + 1) * TILE)
            block = jnp.concatenate([state_ref[n, :, at], state_ref[n + 1, :, at]], axis=0)
            flat = lax.dot_general(eye, block, NT, preferred_element_type=F32)
            for i in range(2):
                low = member_row(cells, m + i) + part * TILE
                turned_ref[low : low + TILE, :] = flat[:, i * 128 : (i + 1) * 128]
    copy.wait()
    for tile in range(eq_ref.shape[1] // TILE):
        at = slice(tile * TILE, (tile + 1) * TILE)
        eq_ref[:, at] = answer_tile(
            lambda i: (cell_ref[0, tile * TILE + i], cell_ref[0, tile * TILE + TILE // 2 + i]),
            w_ref[:, at],
            turned_ref,
            cells,
        )


def answer_kernel(levels, cells, turned_ref, w_ref, before_ref, eq_ref):
    tail = w_ref[112:128, :].astype(F32)
    row = levels - 112
    words = (8.0 * tail[row : row + 1, :] + tail[row + 1 : row + 2, :]).astype(jnp.int32)
    keep = lax.broadcasted_iota(jnp.int32, (128, TILE), 0) < levels
    for tile in range(eq_ref.shape[1] // TILE):
        at = slice(tile * TILE, (tile + 1) * TILE)
        w = w_ref[:, at]
        w = jnp.where(keep, w, jnp.zeros_like(w))
        mid = tile * TILE + TILE // 2
        both = words[:, tile * TILE : mid] + (words[:, mid : mid + TILE // 2] << 16)

        def pair_of(j):
            word = both[0, j]
            return word & 0xFFFF, word >> 16

        eq_ref[:, at] = answer_tile(pair_of, w, turned_ref, cells)


def combine_kernel(firsts, slot_ref, hw_ref, *refs):
    *eq_refs, out_ref = refs
    before = eq_refs.pop(0) if len(eq_refs) > len(firsts) else None
    neigh, obs = slot_ref.shape
    sub = lax.broadcasted_iota(jnp.int32, (8, 128), 0)
    tops, pairs = {}, {}
    for first, ref in zip(firsts, eq_refs):
        for part in range(ref.shape[1] // 128):
            tops[first + part] = ref[0:8, part * 128 : (part + 1) * 128]
            x = ref[8:16, part * 128 : (part + 1) * 128]
            x = x + pltpu.roll(x, 4, 0)
            pairs[first + part] = x + pltpu.roll(x, 2, 0)
    quads = {}
    for q in sorted({i // 4 for i in pairs}):
        x = jnp.zeros((8, 128), F32)
        for j in range(4):
            if 4 * q + j in pairs:
                x = jnp.where(sub >> 1 == j, pairs[4 * q + j], x)
        quads[q] = x
    last = None
    for block in range(obs // 128):
        at = slice(block * 128, (block + 1) * 128)
        a_sum = jnp.zeros((8, 128), F32)
        b_sum = jnp.zeros((8, 128), F32)
        for k in range(neigh):
            s = jnp.broadcast_to(slot_ref[k : k + 1, at], (8, 128))
            low, top = s & 127, s >> 7
            a = jnp.zeros((8, 128), F32)
            for i, x in tops.items():
                a = jnp.where(top == i, jnp.take_along_axis(x, low, axis=1, mode="promise_in_bounds"), a)
            b = jnp.zeros((8, 128), F32)
            top4 = top >> 2
            for i, x in quads.items():
                b = jnp.where(top4 == i, jnp.take_along_axis(x, low, axis=1, mode="promise_in_bounds"), b)
            b = jnp.where((top & 3) == (sub >> 1), b, 0.0)
            h = hw_ref[k : k + 1, at]
            a_sum += a * h
            b_sum += b * h
        b_sum = b_sum + pltpu.roll(b_sum, 4, 0)
        b_sum = b_sum + pltpu.roll(b_sum, 2, 0)
        if before is not None:
            a_sum += before[:, at]
        out_ref[:, at] = a_sum
        last = b_sum if block % 4 == 0 else jnp.where(sub >> 1 >= block % 4, b_sum, last)
        if block % 4 == 3:
            low = obs + block // 4 * 128
            if before is not None:
                last += before[:, low : low + 128]
            out_ref[:, low : low + 128] = last


def unpacked(ref, obs):
    sub = lax.broadcasted_iota(jnp.int32, (8, 128), 0)
    rest = []
    for block in range(obs // 128):
        low = obs + block // 4 * 128
        x = ref[:, low : low + 128]
        if block % 4:
            x = pltpu.roll(x, 8 - 2 * (block % 4), 0)
        rest.append(jnp.where(sub < 2, x, 0.0))
    return jnp.concatenate([ref[:, :obs], jnp.concatenate(rest, axis=1)], axis=0)


def split(x):
    top = x.astype(BF16)
    return top, (x - top.astype(F32)).astype(BF16)


def cov_kernel(members, own_ref, r1_ref, r2_ref, r3_ref, value_ref, error_ref, region_ref, mid_ref, prev_ref, next_ref):
    mem_dev = members // 4
    obs = region_ref.shape[1]
    blocks = [unpacked(ref, obs) for ref in (own_ref, r1_ref, r2_ref, r3_ref)]
    total = blocks[0] + blocks[1] + blocks[2] + blocks[3]
    mean = jnp.sum(total, axis=0, keepdims=True) * (1.0 / members)
    err = error_ref[...]
    inverse = 1.0 / (err * err)
    innov = (value_ref[...] - mean) * inverse
    row = lax.broadcasted_iota(jnp.int32, (16, obs), 0)
    spread = [jnp.where(row < mem_dev, x - mean, 0.0) for x in blocks]
    right = [x * inverse for x in spread]
    right[0] = jnp.where(row == mem_dev, innov, right[0])
    r_top, r_low = split(jnp.concatenate(right, axis=0))
    regions = lax.axis_size("cell") * REG_DEV
    rel = region_ref[...] - (lax.axis_index("cell") - 1) * REG_DEV
    rel = jnp.where(rel < 0, rel + regions, rel)
    rel = jnp.where(rel >= regions, rel - regions, rel)
    region = lax.broadcasted_iota(jnp.int32, (REG_DEV, obs), 0)
    own = spread[0]
    own_low = own - own.astype(BF16).astype(F32)
    for g, out_ref in ((0, prev_ref), (2, next_ref), (1, mid_ref)):
        mask = rel == region + g * REG_DEV
        l_top = jnp.concatenate([jnp.where(mask, own[m : m + 1, :], 0.0) for m in range(mem_dev)], axis=0).astype(BF16)
        l_low = jnp.concatenate([jnp.where(mask, own_low[m : m + 1, :], 0.0) for m in range(mem_dev)], axis=0).astype(BF16)
        d = lax.dot_general(l_top, r_top, NT, preferred_element_type=F32)
        d += lax.dot_general(l_top, r_low, NT, preferred_element_type=F32)
        d += lax.dot_general(l_low, r_top, NT, preferred_element_type=F32)
        out_ref[...] = d


def final_kernel(mid_ref, a_ref, b_ref, cov_ref, proj_ref):
    mem_dev, regions, members = cov_ref.shape
    d = mid_ref[...] + a_ref[...] + b_ref[...]
    width = d.shape[1]
    i = lax.broadcasted_iota(jnp.int32, (width, members), 0)
    j = lax.broadcasted_iota(jnp.int32, (width, members), 1)
    block = lax.axis_index("mem") ^ (i >> 4)
    place = jnp.where(((i & 15) < mem_dev) & (block * mem_dev + (i & 15) == j), 1.0, 0.0)
    cov = jnp.dot(d, place, precision=lax.Precision.HIGHEST, preferred_element_type=F32)
    lane = lax.broadcasted_iota(jnp.int32, (regions, mem_dev), 1)
    proj = jnp.zeros((regions, mem_dev), F32)
    for m in range(mem_dev):
        cov_ref[m] = cov[m * regions : (m + 1) * regions, :]
        proj = jnp.where(lane == m, d[m * regions : (m + 1) * regions, mem_dev : mem_dev + 1], proj)
    proj_ref[...] = proj


def on_device(state, vertical_weight, horizontal_weight, obs_slot, request_cell, obs_value, obs_error, obs_region):
    cells, mem_dev, levels = state.shape
    members = mem_dev * lax.axis_size("mem")
    obs, neigh = obs_slot.shape
    halo = 3 * obs // 4
    state_t = jnp.transpose(state, (1, 2, 0))
    vw_t, hw_t, slot_t = vertical_weight.T, horizontal_weight.T, obs_slot.T
    far = lambda x: pltpu.with_memory_space_constraint(x, pltpu.HBM)
    params = pltpu.CompilerParams(vmem_limit_bytes=16 * 1024 * 1024)

    early = mem_dev - 4
    w_shape = jax.ShapeDtypeStruct((128, halo), BF16)
    inv, vw_near, table, state_near, ask_m2, ask_m1 = pl.pallas_call(
        ask_low_kernel,
        out_shape=[
            pltpu.VMEM((neigh * obs // 128, 128), jnp.int32),
            pltpu.VMEM((levels, obs), BF16),
            pltpu.VMEM((1, neigh * obs), jnp.int32),
            pltpu.VMEM((early, 128, cells), BF16),
            w_shape,
            w_shape,
        ],
        in_specs=[ANY] * 4,
        out_specs=[VMEM] * 6,
        scratch_shapes=[pltpu.VMEM((neigh, obs), jnp.int32), pltpu.SemaphoreType.DMA((3 + early // 2,))],
        compiler_params=params,
        cost_estimate=pl.CostEstimate(flops=2_000_000_000, bytes_accessed=6_000_000, transcendentals=0),
        name="ask_low",
    )(far(slot_t), far(request_cell), far(vw_t), far(state_t))
    w_m2, w_m1 = passed_along(ask_m2, "cell", -2), passed_along(ask_m1, "cell", -1)
    w_own, ask_p1, ask_p2 = pl.pallas_call(
        ask_high_kernel,
        out_shape=[pltpu.VMEM((128, obs), BF16), w_shape, w_shape],
        in_specs=[VMEM] * 3,
        out_specs=[VMEM] * 3,
        compiler_params=params,
        cost_estimate=pl.CostEstimate(flops=2_000_000_000, bytes_accessed=1_000_000, transcendentals=0),
        name="ask_high",
    )(inv, vw_near, table)
    w_p1, w_p2 = passed_along(ask_p1, "cell", 1), passed_along(ask_p2, "cell", 2)
    turned, eq_own = pl.pallas_call(
        own_kernel,
        out_shape=[
            pltpu.VMEM((mem_dev * row_stride(cells), 128), F32),
            pltpu.VMEM((16, obs), F32),
        ],
        in_specs=[VMEM, ANY, ANY, VMEM],
        out_specs=[VMEM] * 2,
        scratch_shapes=[
            pltpu.VMEM((mem_dev - early, 128, cells), BF16),
            pltpu.SMEM((1, obs), jnp.int32),
            pltpu.SemaphoreType.DMA,
            pltpu.SemaphoreType.DMA((2,)),
        ],
        compiler_params=params,
        cost_estimate=pl.CostEstimate(flops=8_000_000_000, bytes_accessed=10_000_000, transcendentals=0),
        name="own",
    )(state_near, far(state_t), far(request_cell), w_own)
    turned = pltpu.with_memory_space_constraint(turned, pltpu.VMEM)
    answer = pl.pallas_call(
        lambda *refs: answer_kernel(levels, cells, *refs),
        out_shape=pltpu.VMEM((16, halo), F32),
        in_specs=[VMEM] * 3,
        out_specs=VMEM,
        compiler_params=params,
        cost_estimate=pl.CostEstimate(flops=2_000_000_000, bytes_accessed=1_000_000, transcendentals=0),
        name="answer",
    )
    sent_m2 = answer(turned, w_m2, eq_own)
    eq_m2 = passed_along(sent_m2, "cell", 2)
    sent_m1 = answer(turned, w_m1, sent_m2)
    eq_m1 = passed_along(sent_m1, "cell", 1)
    sent_p1 = answer(turned, w_p1, sent_m1)
    eq_p1 = passed_along(sent_p1, "cell", -1)
    sent_p2 = answer(turned, w_p2, sent_p1)
    eq_p2 = passed_along(sent_p2, "cell", -2)

    def combine(tables, *before):
        firsts = [obs // 128 + n * halo // 128 if n >= 0 else 0 for n, _ in tables]
        return pl.pallas_call(
            lambda *refs: combine_kernel(firsts, *refs),
            out_shape=jax.ShapeDtypeStruct((8, obs + obs // 4), F32),
            in_specs=[VMEM] * (2 + len(before) + len(tables)),
            out_specs=VMEM,
            compiler_params=params,
            cost_estimate=pl.CostEstimate(flops=1_000_000_000, bytes_accessed=1_000_000, transcendentals=0),
            name="combine",
        )(slot_t, hw_t, *before, *(x for _, x in tables))

    own = combine([(-1, eq_own), (0, eq_m2), (1, eq_m1)])
    own = combine([(2, eq_p1), (3, eq_p2)], own)
    others = [swapped(own, "mem", mask) for mask in (1, 2, 3)]
    wide = 4 * 16
    mid, to_prev, to_next = pl.pallas_call(
        lambda *refs: cov_kernel(members, *refs),
        out_shape=[jax.ShapeDtypeStruct((mem_dev * REG_DEV, wide), F32)] * 3,
        in_specs=[VMEM] * 7,
        out_specs=[VMEM] * 3,
        compiler_params=params,
        name="cov",
    )(own, *others, obs_value.reshape(1, obs), obs_error.reshape(1, obs), obs_region.reshape(1, obs))
    from_prev = passed_along(to_next, "cell", 1)
    from_next = passed_along(to_prev, "cell", -1)
    cov, proj = pl.pallas_call(
        final_kernel,
        out_shape=[
            jax.ShapeDtypeStruct((mem_dev, REG_DEV, members), F32),
            jax.ShapeDtypeStruct((REG_DEV, mem_dev), F32),
        ],
        in_specs=[VMEM] * 3,
        out_specs=[VMEM] * 2,
        compiler_params=params,
        name="final",
    )(mid, from_prev, from_next)
    return (jnp.transpose(cov, (1, 0, 2)), proj)


def solution(mesh):
    in_specs = (
        P("cell", "mem", None),
        P("cell", None),
        P("cell", None),
        P("cell", None),
        P("cell", None),
        P("cell"),
        P("cell"),
        P("cell"),
    )
    out_specs = (P("cell", "mem", None), P("cell", "mem"))
    return jax.shard_map(
        on_device, mesh=mesh, in_specs=in_specs, out_specs=out_specs, check_vma=False
    )
```

```python
import jax
import jax.numpy as jnp
from jax import lax
from jax.experimental import pallas as pl
from jax.experimental.pallas import tpu as pltpu
from jax.sharding import PartitionSpec as P

REG_DEV = 8
TILE = 256
F32 = jnp.float32
BF16 = jnp.bfloat16
NT = (((1,), (1,)), ((), ()))
VMEM = pl.BlockSpec(memory_space=pltpu.VMEM)
ANY = pl.BlockSpec(memory_space=pltpu.HBM)
SMEM = pl.BlockSpec(memory_space=pltpu.SMEM)


def passed_along(x, axis, by):
    devices = lax.axis_size(axis)
    return lax.ppermute(x, axis, [(i, (i + by) % devices) for i in range(devices)])


def swapped(x, axis, mask):
    return lax.ppermute(x, axis, [(i, i ^ mask) for i in range(lax.axis_size(axis))])


def row_stride(cells):
    return cells + 4


def member_row(cells, m):
    return m * row_stride(cells) + (m >= 8)


def slot_owner(slot_ref):
    neigh, obs = slot_ref.shape
    tops = neigh * obs // 128
    o = lax.broadcasted_iota(jnp.int32, (1, obs), 1)
    upper, lower = (o >> 5).astype(F32), (o & 31).astype(F32)
    row_top = lax.broadcasted_iota(jnp.int32, (tops, obs), 0)
    row_low = lax.broadcasted_iota(jnp.int32, (128, obs), 0)
    total = jnp.zeros((2 * tops, 128), F32)
    for k in range(neigh):
        s = slot_ref[k : k + 1, :]
        hit = row_top == (s >> 7)
        lhs = jnp.concatenate(
            [jnp.where(hit, upper, 0.0), jnp.where(hit, lower, 0.0)], axis=0
        ).astype(BF16)
        rhs = jnp.where(row_low == (s & 127), 1.0, 0.0).astype(BF16)
        total += lax.dot_general(lhs, rhs, NT, preferred_element_type=F32)
    return (32.0 * total[:tops] + total[tops:]).astype(jnp.int32)


def slot_weights(inv_ref, vw_ref, tile, table_ref=None):
    levels, obs = vw_ref.shape
    key = jnp.concatenate([inv_ref[2 * tile : 2 * tile + 1, :], inv_ref[2 * tile + 1 : 2 * tile + 2, :]], axis=1)
    ids = lax.broadcasted_iota(jnp.int32, (obs, TILE), 0)
    pick = jnp.where(ids == key, 1.0, 0.0).astype(BF16)
    w = jnp.dot(vw_ref[...], pick, preferred_element_type=F32)
    extra = jnp.zeros((128 - levels, TILE), F32)
    if table_ref is not None:
        cells = table_ref[0:1, tile * TILE : (tile + 1) * TILE]
        sub = lax.broadcasted_iota(jnp.int32, (128 - levels, TILE), 0)
        extra = jnp.where(sub == 0, (cells >> 3).astype(F32), jnp.where(sub == 1, (cells & 7).astype(F32), extra))
    return jnp.concatenate([w, extra], axis=0).astype(BF16)


def ask_low_kernel(slot_hbm, table_hbm, vw_hbm, state_hbm, inv_ref, vw_ref, table_ref, state_ref, *refs):
    *out_refs, slot_ref, sems = refs
    members, levels, cells = state_hbm.shape
    pairs = [(slot_hbm, slot_ref), (vw_hbm, vw_ref), (table_hbm, table_ref)]
    for m in range(0, members, 2):
        pairs.append((state_hbm.at[pl.ds(m, 2)], state_ref.at[pl.ds(m, 2), pl.ds(0, levels), :]))
    for m in range(members):
        state_ref[m, levels:, :] = jnp.zeros((state_ref.shape[1] - levels, cells), BF16)
    copies = [pltpu.make_async_copy(src, dst, sems.at[i]) for i, (src, dst) in enumerate(pairs)]
    for copy in copies:
        copy.start()
    copies[0].wait()
    inv_ref[...] = slot_owner(slot_ref)
    copies[1].wait()
    copies[2].wait()
    halo_weights(inv_ref, vw_ref, table_ref, out_refs, (0, 1))
    for copy in copies[3:]:
        copy.wait()


def ask_high_kernel(inv_ref, vw_ref, table_ref, own_ref, *out_refs):
    halo_weights(inv_ref, vw_ref, table_ref, out_refs, (2, 3))
    for tile in range(own_ref.shape[1] // TILE):
        own_ref[:, tile * TILE : (tile + 1) * TILE] = slot_weights(inv_ref, vw_ref, tile)


def halo_weights(inv_ref, vw_ref, table_ref, out_refs, numbers):
    obs = vw_ref.shape[1]
    for out, number in zip(out_refs, numbers):
        count = out.shape[1] // TILE
        for part in range(count):
            tile = obs // TILE + number * count + part
            out[:, part * TILE : (part + 1) * TILE] = slot_weights(inv_ref, vw_ref, tile, table_ref)


def answer_tile(pair_of, w, turned_ref, cells_dim):
    S, rest = row_stride(cells_dim), member_row(cells_dim, 8)
    half = TILE // 2
    lane = lax.broadcasted_iota(jnp.int32, (8, 128), 1)
    near = lane - (lax.broadcasted_iota(jnp.int32, (8, 128), 0) >> 1)
    wide = lax.broadcasted_iota(jnp.int32, (128, TILE), 1)
    zero = jnp.zeros_like(w)
    rhs = jnp.concatenate([jnp.where(wide < half, w, zero), jnp.where(wide < half, zero, w)], axis=0)
    parts = []
    for o in range(half // 8):
        sides = []
        pairs = [pair_of(8 * o + j) for j in range(8)]
        for h in range(2):
            a_rows, b_rows = [], []
            for j in range(8):
                c = pairs[j][h]
                a_rows.append(turned_ref[pl.ds(c, 8, stride=S), :])
                b_rows.append(turned_ref[pl.ds(c + rest, 2, stride=S), :])
            sides.append(jnp.concatenate(a_rows + b_rows, axis=0).astype(BF16))
        parts.append(jnp.concatenate(sides, axis=1))
    d = jnp.dot(jnp.concatenate(parts, axis=0), rhs, preferred_element_type=F32)
    out_a = [jnp.zeros((8, 128), F32)] * 2
    out_b = [jnp.zeros((8, 128), F32)] * 2
    for o in range(half // 8):
        for j in range(8):
            low = 80 * o + 8 * j
            hit = lane == 8 * o + j
            for h in range(2):
                out_a[h] = jnp.where(hit, d[low : low + 8, h * half : (h + 1) * half], out_a[h])
        for i in range(2):
            low = 80 * o + 64 + 8 * i
            hit = near == 8 * o + 4 * i
            for h in range(2):
                out_b[h] = jnp.where(hit, d[low : low + 8, h * half : (h + 1) * half], out_b[h])
    return jnp.concatenate([jnp.concatenate(out_a, axis=1), jnp.concatenate(out_b, axis=1)], axis=0)


def own_kernel(state_ref, table_hbm, w_ref, turned_ref, eq_ref, cell_ref, cell_sem):
    members, levels, cells = state_ref.shape
    copy = pltpu.make_async_copy(table_hbm.at[:, pl.ds(0, eq_ref.shape[1])], cell_ref, cell_sem)
    copy.start()
    r = lax.broadcasted_iota(jnp.int32, (TILE, TILE), 0)
    eye = jnp.where(r == lax.broadcasted_iota(jnp.int32, (TILE, TILE), 1), 1.0, 0.0).astype(BF16)
    for m in range(0, members, 2):
        for part in range(cells // TILE):
            at = slice(part * TILE, (part + 1) * TILE)
            block = jnp.concatenate([state_ref[m, :, at], state_ref[m + 1, :, at]], axis=0)
            flat = lax.dot_general(eye, block, NT, preferred_element_type=F32)
            for i in range(2):
                low = member_row(cells, m + i) + part * TILE
                turned_ref[low : low + TILE, :] = flat[:, i * 128 : (i + 1) * 128]
    copy.wait()
    for tile in range(eq_ref.shape[1] // TILE):
        at = slice(tile * TILE, (tile + 1) * TILE)
        eq_ref[:, at] = answer_tile(
            lambda i: (cell_ref[0, tile * TILE + i], cell_ref[0, tile * TILE + TILE // 2 + i]),
            w_ref[:, at],
            turned_ref,
            cells,
        )


def answer_kernel(levels, cells, turned_ref, w_ref, before_ref, eq_ref):
    tail = w_ref[112:128, :].astype(F32)
    row = levels - 112
    words = (8.0 * tail[row : row + 1, :] + tail[row + 1 : row + 2, :]).astype(jnp.int32)
    keep = lax.broadcasted_iota(jnp.int32, (128, TILE), 0) < levels
    for tile in range(eq_ref.shape[1] // TILE):
        at = slice(tile * TILE, (tile + 1) * TILE)
        w = w_ref[:, at]
        w = jnp.where(keep, w, jnp.zeros_like(w))
        mid = tile * TILE + TILE // 2
        both = words[:, tile * TILE : mid] + (words[:, mid : mid + TILE // 2] << 16)

        def pair_of(j):
            word = both[0, j]
            return word & 0xFFFF, word >> 16

        eq_ref[:, at] = answer_tile(pair_of, w, turned_ref, cells)


def combine_kernel(firsts, slot_ref, hw_ref, *refs):
    *eq_refs, out_ref = refs
    before = eq_refs.pop(0) if len(eq_refs) > len(firsts) else None
    neigh, obs = slot_ref.shape
    sub = lax.broadcasted_iota(jnp.int32, (8, 128), 0)
    tops, pairs = {}, {}
    for first, ref in zip(firsts, eq_refs):
        for part in range(ref.shape[1] // 128):
            tops[first + part] = ref[0:8, part * 128 : (part + 1) * 128]
            x = ref[8:16, part * 128 : (part + 1) * 128]
            x = x + pltpu.roll(x, 4, 0)
            pairs[first + part] = x + pltpu.roll(x, 2, 0)
    quads = {}
    for q in sorted({i // 4 for i in pairs}):
        x = jnp.zeros((8, 128), F32)
        for j in range(4):
            if 4 * q + j in pairs:
                x = jnp.where(sub >> 1 == j, pairs[4 * q + j], x)
        quads[q] = x
    last = None
    for block in range(obs // 128):
        at = slice(block * 128, (block + 1) * 128)
        a_sum = jnp.zeros((8, 128), F32)
        b_sum = jnp.zeros((8, 128), F32)
        for k in range(neigh):
            s = jnp.broadcast_to(slot_ref[k : k + 1, at], (8, 128))
            low, top = s & 127, s >> 7
            a = jnp.zeros((8, 128), F32)
            for i, x in tops.items():
                a = jnp.where(top == i, jnp.take_along_axis(x, low, axis=1, mode="promise_in_bounds"), a)
            b = jnp.zeros((8, 128), F32)
            top4 = top >> 2
            for i, x in quads.items():
                b = jnp.where(top4 == i, jnp.take_along_axis(x, low, axis=1, mode="promise_in_bounds"), b)
            b = jnp.where((top & 3) == (sub >> 1), b, 0.0)
            h = hw_ref[k : k + 1, at]
            a_sum += a * h
            b_sum += b * h
        b_sum = b_sum + pltpu.roll(b_sum, 4, 0)
        b_sum = b_sum + pltpu.roll(b_sum, 2, 0)
        if before is not None:
            a_sum += before[:, at]
        out_ref[:, at] = a_sum
        last = b_sum if block % 4 == 0 else jnp.where(sub >> 1 >= block % 4, b_sum, last)
        if block % 4 == 3:
            low = obs + block // 4 * 128
            if before is not None:
                last += before[:, low : low + 128]
            out_ref[:, low : low + 128] = last


def unpacked(ref, obs):
    sub = lax.broadcasted_iota(jnp.int32, (8, 128), 0)
    rest = []
    for block in range(obs // 128):
        low = obs + block // 4 * 128
        x = ref[:, low : low + 128]
        if block % 4:
            x = pltpu.roll(x, 8 - 2 * (block % 4), 0)
        rest.append(jnp.where(sub < 2, x, 0.0))
    return jnp.concatenate([ref[:, :obs], jnp.concatenate(rest, axis=1)], axis=0)


def split(x):
    top = x.astype(BF16)
    return top, (x - top.astype(F32)).astype(BF16)


def cov_kernel(members, own_ref, r1_ref, r2_ref, r3_ref, value_ref, error_ref, region_ref, mid_ref, prev_ref, next_ref):
    mem_dev = members // 4
    obs = region_ref.shape[1]
    blocks = [unpacked(ref, obs) for ref in (own_ref, r1_ref, r2_ref, r3_ref)]
    total = blocks[0] + blocks[1] + blocks[2] + blocks[3]
    mean = jnp.sum(total, axis=0, keepdims=True) * (1.0 / members)
    err = error_ref[...]
    inverse = 1.0 / (err * err)
    innov = (value_ref[...] - mean) * inverse
    row = lax.broadcasted_iota(jnp.int32, (16, obs), 0)
    spread = [jnp.where(row < mem_dev, x - mean, 0.0) for x in blocks]
    right = [x * inverse for x in spread]
    right[0] = jnp.where(row == mem_dev, innov, right[0])
    r_top, r_low = split(jnp.concatenate(right, axis=0))
    regions = lax.axis_size("cell") * REG_DEV
    rel = region_ref[...] - (lax.axis_index("cell") - 1) * REG_DEV
    rel = jnp.where(rel < 0, rel + regions, rel)
    rel = jnp.where(rel >= regions, rel - regions, rel)
    region = lax.broadcasted_iota(jnp.int32, (REG_DEV, obs), 0)
    own = spread[0]
    own_low = own - own.astype(BF16).astype(F32)
    for g, out_ref in ((0, prev_ref), (2, next_ref), (1, mid_ref)):
        mask = rel == region + g * REG_DEV
        l_top = jnp.concatenate([jnp.where(mask, own[m : m + 1, :], 0.0) for m in range(mem_dev)], axis=0).astype(BF16)
        l_low = jnp.concatenate([jnp.where(mask, own_low[m : m + 1, :], 0.0) for m in range(mem_dev)], axis=0).astype(BF16)
        d = lax.dot_general(l_top, r_top, NT, preferred_element_type=F32)
        d += lax.dot_general(l_top, r_low, NT, preferred_element_type=F32)
        d += lax.dot_general(l_low, r_top, NT, preferred_element_type=F32)
        out_ref[...] = d


def final_kernel(mid_ref, a_ref, b_ref, cov_ref, proj_ref):
    mem_dev, regions, members = cov_ref.shape
    d = mid_ref[...] + a_ref[...] + b_ref[...]
    width = d.shape[1]
    i = lax.broadcasted_iota(jnp.int32, (width, members), 0)
    j = lax.broadcasted_iota(jnp.int32, (width, members), 1)
    block = lax.axis_index("mem") ^ (i >> 4)
    place = jnp.where(((i & 15) < mem_dev) & (block * mem_dev + (i & 15) == j), 1.0, 0.0)
    cov = jnp.dot(d, place, precision=lax.Precision.HIGHEST, preferred_element_type=F32)
    lane = lax.broadcasted_iota(jnp.int32, (regions, mem_dev), 1)
    proj = jnp.zeros((regions, mem_dev), F32)
    for m in range(mem_dev):
        cov_ref[m] = cov[m * regions : (m + 1) * regions, :]
        proj = jnp.where(lane == m, d[m * regions : (m + 1) * regions, mem_dev : mem_dev + 1], proj)
    proj_ref[...] = proj


def on_device(state, vertical_weight, horizontal_weight, obs_slot, request_cell, obs_value, obs_error, obs_region):
    cells, mem_dev, levels = state.shape
    members = mem_dev * lax.axis_size("mem")
    obs, neigh = obs_slot.shape
    halo = 3 * obs // 4
    state_t = jnp.transpose(state, (1, 2, 0))
    vw_t, hw_t, slot_t = vertical_weight.T, horizontal_weight.T, obs_slot.T
    far = lambda x: pltpu.with_memory_space_constraint(x, pltpu.HBM)
    params = pltpu.CompilerParams(vmem_limit_bytes=16 * 1024 * 1024)

    w_shape = jax.ShapeDtypeStruct((128, halo), BF16)
    inv, vw_near, table, state_near, ask_m2, ask_m1 = pl.pallas_call(
        ask_low_kernel,
        out_shape=[
            pltpu.VMEM((neigh * obs // 128, 128), jnp.int32),
            pltpu.VMEM((levels, obs), BF16),
            pltpu.VMEM((1, neigh * obs), jnp.int32),
            pltpu.VMEM((mem_dev, 128, cells), BF16),
            w_shape,
            w_shape,
        ],
        in_specs=[ANY] * 4,
        out_specs=[VMEM] * 6,
        scratch_shapes=[pltpu.VMEM((neigh, obs), jnp.int32), pltpu.SemaphoreType.DMA((3 + mem_dev // 2,))],
        compiler_params=params,
        cost_estimate=pl.CostEstimate(flops=2_000_000_000, bytes_accessed=6_000_000, transcendentals=0),
        name="ask_low",
    )(far(slot_t), far(request_cell), far(vw_t), far(state_t))
    w_m2, w_m1 = passed_along(ask_m2, "cell", -2), passed_along(ask_m1, "cell", -1)
    w_own, ask_p1, ask_p2 = pl.pallas_call(
        ask_high_kernel,
        out_shape=[pltpu.VMEM((128, obs), BF16), w_shape, w_shape],
        in_specs=[VMEM] * 3,
        out_specs=[VMEM] * 3,
        compiler_params=params,
        cost_estimate=pl.CostEstimate(flops=2_000_000_000, bytes_accessed=1_000_000, transcendentals=0),
        name="ask_high",
    )(inv, vw_near, table)
    w_p1, w_p2 = passed_along(ask_p1, "cell", 1), passed_along(ask_p2, "cell", 2)
    turned, eq_own = pl.pallas_call(
        own_kernel,
        out_shape=[
            pltpu.VMEM((mem_dev * row_stride(cells), 128), F32),
            pltpu.VMEM((16, obs), F32),
        ],
        in_specs=[VMEM, ANY, VMEM],
        out_specs=[VMEM] * 2,
        scratch_shapes=[pltpu.SMEM((1, obs), jnp.int32), pltpu.SemaphoreType.DMA],
        compiler_params=params,
        cost_estimate=pl.CostEstimate(flops=8_000_000_000, bytes_accessed=10_000_000, transcendentals=0),
        name="own",
    )(state_near, far(request_cell), w_own)
    turned = pltpu.with_memory_space_constraint(turned, pltpu.VMEM)
    answer = pl.pallas_call(
        lambda *refs: answer_kernel(levels, cells, *refs),
        out_shape=pltpu.VMEM((16, halo), F32),
        in_specs=[VMEM] * 3,
        out_specs=VMEM,
        compiler_params=params,
        cost_estimate=pl.CostEstimate(flops=2_000_000_000, bytes_accessed=1_000_000, transcendentals=0),
        name="answer",
    )
    sent_m2 = answer(turned, w_m2, eq_own)
    eq_m2 = passed_along(sent_m2, "cell", 2)
    sent_m1 = answer(turned, w_m1, sent_m2)
    eq_m1 = passed_along(sent_m1, "cell", 1)
    sent_p1 = answer(turned, w_p1, sent_m1)
    eq_p1 = passed_along(sent_p1, "cell", -1)
    sent_p2 = answer(turned, w_p2, sent_p1)
    eq_p2 = passed_along(sent_p2, "cell", -2)

    def combine(tables, *before):
        firsts = [obs // 128 + n * halo // 128 if n >= 0 else 0 for n, _ in tables]
        return pl.pallas_call(
            lambda *refs: combine_kernel(firsts, *refs),
            out_shape=jax.ShapeDtypeStruct((8, obs + obs // 4), F32),
            in_specs=[VMEM] * (2 + len(before) + len(tables)),
            out_specs=VMEM,
            compiler_params=params,
            cost_estimate=pl.CostEstimate(flops=1_000_000_000, bytes_accessed=1_000_000, transcendentals=0),
            name="combine",
        )(slot_t, hw_t, *before, *(x for _, x in tables))

    own = combine([(-1, eq_own), (0, eq_m2), (1, eq_m1)])
    own = combine([(2, eq_p1), (3, eq_p2)], own)
    others = [swapped(own, "mem", mask) for mask in (1, 2, 3)]
    wide = 4 * 16
    mid, to_prev, to_next = pl.pallas_call(
        lambda *refs: cov_kernel(members, *refs),
        out_shape=[jax.ShapeDtypeStruct((mem_dev * REG_DEV, wide), F32)] * 3,
        in_specs=[VMEM] * 7,
        out_specs=[VMEM] * 3,
        compiler_params=params,
        name="cov",
    )(own, *others, obs_value.reshape(1, obs), obs_error.reshape(1, obs), obs_region.reshape(1, obs))
    from_prev = passed_along(to_next, "cell", 1)
    from_next = passed_along(to_prev, "cell", -1)
    cov, proj = pl.pallas_call(
        final_kernel,
        out_shape=[
            jax.ShapeDtypeStruct((mem_dev, REG_DEV, members), F32),
            jax.ShapeDtypeStruct((REG_DEV, mem_dev), F32),
        ],
        in_specs=[VMEM] * 3,
        out_specs=[VMEM] * 2,
        compiler_params=params,
        name="final",
    )(mid, from_prev, from_next)
    return (jnp.transpose(cov, (1, 0, 2)), proj)


def solution(mesh):
    in_specs = (
        P("cell", "mem", None),
        P("cell", None),
        P("cell", None),
        P("cell", None),
        P("cell", None),
        P("cell"),
        P("cell"),
        P("cell"),
    )
    out_specs = (P("cell", "mem", None), P("cell", "mem"))
    return jax.shard_map(
        on_device, mesh=mesh, in_specs=in_specs, out_specs=out_specs, check_vma=False
    )
```
